32 devices in a mesh: groups: 2 (over x), rows: 16 (over z, y, core).
Axes of the slice: x: 2, y: 2, z: 4, core: 2. Of those that a mesh axis runs over, the one named last changes fastest.
Arguments:
- slide_band: bfloat16 [96, 256, 512], P(None, ('groups', 'rows')), parts along dimension 1, may hold values from -8 to 8
- tissue_flags: int32 [32, 64], P(('groups', 'rows')), parts along dimension 0, may hold values from 0 to 1, as said below
- stain_index: int32 [32, 64], P(('groups', 'rows')), parts along dimension 0, may hold values from 0 to 3
- stain_gain: float32 [4, 96], replicated, may hold values from 0.5 to 2
- conv_weights: bfloat16 [3, 9, 96, 96], replicated, may hold values from -0.21875 to 0.21875
- norm_gain: float32 [3, 96], replicated, may hold values from 0.5 to 2
- norm_bias: float32 [3, 96], replicated, may hold values from -3 to 3
Outputs:
- features: bfloat16 [96, 256, 512], P(None, ('groups', 'rows')), parts along dimension 1
The draws below stay inside these ranges and needn't reach their ends.
There are 2 independent parts, one for each index of `groups`. The reference program is written for one: setup_inputs(seed, part) draws one part's arguments, and reference() takes and returns one part's arrays. A program takes and returns all parts, laid end to end along the dimension named above; an argument that names none is the same for every part. Nothing has to cross between parts.
Inputs may be any that keep to these rules, and one draw needn't show every extreme that they name: `tissue_flags`: in every aligned block of 1 tile rows, the first tile of the block's first tile row is tissue.
All inputs are finite; a program needn't handle non-finite values.
Results may differ from the reference program's by a relative error of at most 0.018.
Values may be sent and summed in bfloat16 or wider, within the bound.
A program may use at most 64 MiB of HBM per device.

```python
import math
import jax
import jax.numpy as jnp
from jax import lax

CHANNELS = 96
LAYERS = 3
TILE = 8
STAINS = 4
BAND_ROWS = 8
COLUMNS = 512
HEIGHT = 128


def draw_slide_band(key, part):
    first_key = jax.random.fold_in(jax.random.fold_in(key, 11), 0)
    position = jnp.arange(HEIGHT, dtype=jnp.float32) / max(HEIGHT - 1, 1)
    base = jax.random.normal(first_key, (CHANNELS, HEIGHT, COLUMNS), jnp.float32)
    values = base * (0.6 + 1.2 * position)[None, :, None]
    return jnp.clip(values, -8.0, 8.0).astype(jnp.bfloat16)


def draw_tissue_flags(key, part):
    tile_rows = HEIGHT // TILE
    tile_cols = COLUMNS // TILE
    rolled = jax.random.randint(jax.random.fold_in(key, 23), (tile_rows, tile_cols), 0, 1000)
    row_ids = jnp.arange(tile_rows, dtype=jnp.int32)[:, None]
    col_ids = jnp.arange(tile_cols, dtype=jnp.int32)[None, :]
    threshold = 250 + 700 * row_ids // max(tile_rows - 1, 1)
    flags = (rolled < threshold).astype(jnp.int32)
    block_rows = BAND_ROWS // TILE
    forced = (row_ids % block_rows == 0) & (col_ids == 0)
    return jnp.where(forced, 1, flags).astype(jnp.int32)


def plant(values, key, low, largest):
    extent = values.shape
    index_at = [jax.random.randint(jax.random.fold_in(key, axis), (), 0, extent[axis]) for axis in range(len(extent))]
    values = values.at[tuple(index_at)].set(low)
    longest = extent.index(max(extent))
    index_at[longest] = (index_at[longest] + 1) % extent[longest]
    return values.at[tuple(index_at)].set(largest)


def gaussian(own_key, extent, spread, limit, kind=jnp.bfloat16):
    return jnp.clip(spread * jax.random.normal(own_key, extent, jnp.float32), -limit, limit).astype(kind)


def setup_inputs(seed: int = 0, part: int = 0) -> dict:
    key_list = jax.random.split(jax.random.key(seed), 8)
    own_keys = jax.random.split(jax.random.fold_in(key_list[7], part), 8)
    return {
        "slide_band": draw_slide_band(jax.random.fold_in(jax.random.fold_in(key_list[7], part), 71), part),
        "tissue_flags": draw_tissue_flags(jax.random.fold_in(jax.random.fold_in(key_list[7], part), 71), part),
        "stain_index": plant(jax.random.randint(own_keys[2], (HEIGHT // TILE, COLUMNS // TILE), 0, STAINS), jax.random.fold_in(own_keys[2], 1), 0, STAINS - 1).astype(jnp.int32),
        "stain_gain": jnp.clip(jnp.exp(jax.random.uniform(key_list[3], (STAINS, CHANNELS), jnp.float32, math.log(0.5), math.log(2.0))), 0.5, 2.0),
        "conv_weights": gaussian(key_list[4], (LAYERS, 9, CHANNELS, CHANNELS), (9 * CHANNELS) ** -0.5, 0.21875),
        "norm_gain": jnp.clip(jnp.exp(jax.random.uniform(key_list[5], (LAYERS, CHANNELS), jnp.float32, math.log(0.5), math.log(2.0))), 0.5, 2.0),
        "norm_bias": gaussian(key_list[6], (LAYERS, CHANNELS), 0.5, 3.0, jnp.float32),
    }


epsilon = 1e-05

def spread_tiles(tiles):
    return jnp.repeat(jnp.repeat(tiles, TILE, axis=-2), TILE, axis=-1)

def conv_layer(inputs, weights, spacing):
    height = inputs.shape[1]
    col_count = inputs.shape[2]
    padded = jnp.pad(inputs, ((0, 0), (spacing, spacing), (spacing, spacing)))
    running = jnp.zeros((weights.shape[1], height, col_count), jnp.float32)
    for kernel_tap in range(9):
        row_tap = kernel_tap // 3
        col_tap = kernel_tap % 3
        window = padded[:, row_tap * spacing:row_tap * spacing + height, col_tap * spacing:col_tap * spacing + col_count]
        running = running + jnp.einsum('oc,chw->ohw', weights[kernel_tap].astype(jnp.float32), window)
    return running

def reference(slide_band, tissue_flags, stain_index, stain_gain, conv_weights, norm_gain, norm_bias):
    pixels = spread_tiles(tissue_flags.astype(jnp.float32))
    stain_scale = spread_tiles(jnp.transpose(stain_gain[stain_index], (2, 0, 1)))
    current = (slide_band.astype(jnp.float32) * stain_scale * pixels[None]).astype(jnp.bfloat16)
    count_all = jnp.sum(pixels)
    for layer_index in range(LAYERS):
        spacing = 2 ** layer_index
        response = conv_layer(current.astype(jnp.float32), conv_weights[layer_index], spacing)
        average = lax.optimization_barrier(jnp.sum(response * pixels[None], axis=(1, 2))) / count_all
        centred = response - average[:, None, None]
        variance = lax.optimization_barrier(jnp.sum(centred * centred * pixels[None], axis=(1, 2))) / count_all
        scaled = norm_gain[layer_index][:, None, None] * centred * lax.rsqrt(variance + epsilon)[:, None, None] + norm_bias[layer_index][:, None, None]
        current = (jnp.maximum(scaled, 0.0) * pixels[None]).astype(jnp.bfloat16)
    return current
```

```python
import functools

import jax
import jax.numpy as jnp
from jax import lax
from jax.experimental import pallas as pl
from jax.experimental.pallas import tpu as pltpu
from jax.sharding import PartitionSpec as P

LAYERS = 3
TILE = 8
STAINS = 4
REACH = 2**LAYERS - 1
EPSILON = 1e-05
NEAR = 4
MESH = pl.DeviceIdType.MESH
scope = jax.named_scope


def rounds(peers):
    out = []
    reach = NEAR
    while reach < peers - 1:
        out.append(reach)
        reach *= 2
    return tuple(out)


def stack(
    peers,
    slide_ref,
    flags_ref,
    index_ref,
    stain_ref,
    weights_ref,
    gain_ref,
    bias_ref,
    own_ref,
    norm_ref,
    mask_ref,
    slide,
    flags,
    index,
    stain,
    gains,
    biases,
    weights,
    turned,
    scale,
    x0,
    x1,
    x2,
    halo,
    taps,
    masks,
    flag_out,
    flag_in,
    tally_out,
    tally_in,
    edge_send,
    edge_recv,
    tally_send,
    tally_recv,
    local_sem,
    far_sem,
):
    channels, rows, cols = slide_ref.shape
    tiles = flags_ref.shape[1]
    bf16, f32 = jnp.bfloat16, jnp.float32
    me = lax.axis_index("rows")
    has_up = me > 0
    has_down = me < peers - 1
    inputs = (x0, x1, x2)
    first = (REACH, REACH - 1, REACH - 3)
    chunks = cols // 128
    barrier = pltpu.get_barrier_semaphore()

    fetches = {}
    for n, (name, source, target) in enumerate(
        (
            ("flags", flags_ref, flags),
            ("index", index_ref, index),
            ("stain", stain_ref, stain),
            ("slide", slide_ref, slide),
            ("weights", weights_ref, weights),
            ("gain", gain_ref, gains),
            ("bias", bias_ref, biases),
        )
    ):
        fetches[name] = pltpu.make_async_copy(source, target, local_sem.at[n])
        fetches[name].start()

    flag_in[...] = jnp.zeros_like(flag_in)

    def other_side(distance, side):
        there = me - distance if side == 0 else me + distance
        exists = there >= 0 if side == 0 else there < peers
        return there, exists

    for distance in range(1, NEAR + 1):
        for side in range(2):
            there, exists = other_side(distance, side)

            @pl.when(exists)
            def _():
                pl.semaphore_signal(barrier, inc=1, device_id={"rows": there}, device_id_type=MESH)

    def far_signal(n):
        for side in range(2):
            there, exists = other_side(rounds(peers)[n], side)

            @pl.when(exists)
            def _():
                pl.semaphore_signal(
                    far_sem.at[n, 1 - side], inc=1, device_id={"rows": there}, device_id_type=MESH
                )

    def far_wait(n):
        for side in range(2):
            _, exists = other_side(rounds(peers)[n], side)

            @pl.when(exists)
            def _():
                pl.semaphore_wait(far_sem.at[n, side], 1)

    spread = (
        lax.broadcasted_iota(jnp.int32, (128, cols), 1) // TILE
        == lax.broadcasted_iota(jnp.int32, (128, cols), 0)
    ).astype(f32)
    eye = lax.broadcasted_iota(jnp.int32, (channels, channels), 0) == lax.broadcasted_iota(
        jnp.int32, (channels, channels), 1
    )

    def column(row):
        return jnp.sum(jnp.where(eye, row, 0.0), axis=1, keepdims=True)

    def as_row(col):
        return jnp.sum(jnp.where(eye, col, 0.0), axis=0, keepdims=True)

    def widen(values):
        return jnp.dot(values, spread, preferred_element_type=f32)

    flag_out[...] = jnp.zeros_like(flag_out)

    with scope("a0_small"):
        fetches["flags"].wait()
        fetches["index"].wait()
        fetches["stain"].wait()
    with scope("a1_scale"):
        flag_out[:, 0:tiles] = jnp.broadcast_to(
            flags[...].astype(f32), (flag_out.shape[0], tiles)
        )
        masks[0] = widen(flag_out[...])
        mask_ref[...] = masks[0]
        classes = jnp.dot(
            jnp.broadcast_to(index[...].astype(f32), (8, tiles)),
            spread[0:tiles],
            preferred_element_type=f32,
        )[0:1]
        factor = jnp.zeros((channels, cols), f32)
        for kind in range(STAINS):
            factor = jnp.where(classes == kind, column(stain[kind : kind + 1, :]), factor)
        scale[...] = factor * masks[0, 0:1, :]
    with scope("a2_slide"):
        fetches["slide"].wait()
    with scope("a3_turn"):
        for at in range(chunks):
            turned[at] = (
                slide[:, :, at * 128 : (at + 1) * 128].astype(f32).reshape(channels * rows, 128)
            )

    lane = lax.broadcasted_iota(jnp.int32, (1, 128), 1)

    def shifts(values, spacing):
        inside = (lane >= spacing).astype(f32).astype(bf16)
        left = pltpu.roll(values, spacing, 1)
        left = jnp.concatenate([left[:, 0:128] * inside, left[:, 128:]], axis=1)
        inside = (lane < 128 - spacing).astype(f32).astype(bf16)
        right = pltpu.roll(values, cols - spacing, 1)
        right = jnp.concatenate([right[:, : cols - 128], right[:, cols - 128 :] * inside], axis=1)
        return left, right

    def place(buffer, row, values, spacing):
        buffer[1, row] = values
        buffer[0, row], buffer[2, row] = shifts(values, spacing)

    def load_row(row):
        values = jnp.concatenate(
            [turned[at, pl.ds(row, channels, stride=rows), :] for at in range(chunks)], axis=1
        )
        return (values * scale[...]).astype(bf16)

    with scope("a4_edge_rows"):
        for row in (0, rows - 1):
            place(x0, first[0] + row, load_row(row), 1)

    def edge_copy(piece, side):
        if piece == REACH:
            source, target = flag_out, flag_in.at[1 - side]
        else:
            start = REACH + piece if side == 0 else REACH + rows - 1 - piece
            land = REACH + rows + piece if side == 0 else REACH - 1 - piece
            source, target = x0.at[1, start], x0.at[1, land]
        return pltpu.make_async_remote_copy(
            src_ref=source,
            dst_ref=target,
            send_sem=edge_send.at[piece, side],
            recv_sem=edge_recv.at[piece, side],
            device_id={"rows": me - 1 if side == 0 else me + 1},
            device_id_type=MESH,
        )

    def on_edges(piece, act, up, down):
        @pl.when(up)
        def _():
            act(edge_copy(piece, 0))

        @pl.when(down)
        def _():
            act(edge_copy(piece, 1))

    def send_edge(piece):
        on_edges(piece, lambda copy: copy.start(), has_up, has_down)

    def sent_edge(piece):
        on_edges(piece, lambda copy: copy.wait_send(), has_up, has_down)

    def take_edge(piece):
        on_edges(piece, lambda copy: copy.wait_recv(), has_down, has_up)

    with scope("a5_barrier"):
        near = jnp.minimum(me, NEAR) + jnp.minimum(peers - 1 - me, NEAR)
        pl.semaphore_wait(barrier, near)
    with scope("a6_send"):
        send_edge(0)
        send_edge(REACH)
        far = rounds(peers)
        if far:
            far_signal(0)

    with scope("a7_rows"):
        for row in range(1, rows - 1):
            place(x0, first[0] + row, load_row(row), 1)
        send_edge(1)

        @pl.when(jnp.logical_not(has_up))
        def _():
            x0[1, 0:REACH] = jnp.zeros((REACH, channels, cols), bf16)

        @pl.when(jnp.logical_not(has_down))
        def _():
            x0[1, REACH + rows : 2 * REACH + rows] = jnp.zeros((REACH, channels, cols), bf16)

    def set_taps(layer):
        for tap in range(9):
            taps[layer, :, tap * channels : (tap + 1) * channels] = weights[layer, tap]

    with scope("a8_taps"):
        fetches["weights"].wait()
        set_taps(0)

    def place_shifts(row):
        x0[0, row], x0[2, row] = shifts(x0[1, row], 1)

    def conv_row(layer, row):
        spacing = 2**layer
        source = inputs[layer]
        window = jnp.concatenate(
            [
                source[b, first[layer] + row + (a - 1) * spacing]
                for a in range(3)
                for b in range(3)
            ],
            axis=0,
        )
        return jnp.dot(taps[layer], window, preferred_element_type=f32)

    def halo_at(row):
        return row + REACH - 1 if row < 0 else row - rows + REACH - 1

    def put(row, values):
        if 0 <= row < rows:
            own_ref[row] = values
        else:
            halo[halo_at(row)] = values

    def get(row):
        return own_ref[row] if 0 <= row < rows else halo[halo_at(row)]

    def fold(values):
        total = values[:, 0:128]
        for at in range(128, cols, 128):
            total = total + values[:, at : at + 128]
        return total

    def own_row(layer, row, carry):
        sums, squares = carry
        own = conv_row(layer, row)
        own_ref[row] = own
        masked = own * masks[0, 0:1, :]
        return sums + fold(masked), squares + fold(masked * own)

    def tally(layer, carry):
        sums, squares = carry
        tally_out[layer, 0:1, 0:channels] = as_row(jnp.sum(sums, axis=1, keepdims=True))
        tally_out[layer, 1:2, 0:channels] = as_row(jnp.sum(squares, axis=1, keepdims=True))
        pixels = jnp.sum(masks[0, 0:1, :], axis=1, keepdims=True) * rows
        tally_out[layer, :, channels:] = jnp.broadcast_to(pixels, (2, 128 - channels))
        tally_in[layer, me] = tally_out[layer]

    def tally_copy(layer, step, other, slot):
        return pltpu.make_async_remote_copy(
            src_ref=tally_out.at[layer],
            dst_ref=tally_in.at[layer, slot],
            send_sem=tally_send.at[layer, step],
            recv_sem=tally_recv.at[layer, slot],
            device_id={"rows": other},
            device_id_type=MESH,
        )

    def send_tally(layer):
        def one(turn, carry):
            step = peers - turn

            @pl.when(me + step < peers)
            def _():
                tally_copy(layer, step, me + step, me).start()

            @pl.when(me >= step)
            def _():
                tally_copy(layer, peers - step, me - step, me).start()

            return carry

        lax.fori_loop(1, peers, one, 0)

    def take_tally(layer):
        def one(step, carry):
            other = lax.rem(me + step, peers)
            tally_copy(layer, step, other, other).wait_recv()
            return carry

        lax.fori_loop(1, peers, one, 0)
        total = jnp.sum(tally_in[layer], axis=0)
        count = total[0:1, channels : channels + 1]
        average = total[0:1, 0:channels] / count
        variance = jnp.maximum(total[1:2, 0:channels] / count - average * average, 0.0)
        factor = gains[layer : layer + 1, :] * lax.rsqrt(variance + EPSILON)
        return column(average), column(factor), column(biases[layer : layer + 1, :])

    def finish_row(layer, row, norm):
        average, factor, bias = norm
        which = 0 if 0 <= row < rows else 1 if row < 0 else 2
        scaled = ((get(row) - average) * factor + bias).astype(bf16)
        mask = masks[which, 0:1, :].astype(bf16)
        values = jnp.maximum(scaled, jnp.zeros((), bf16)) * mask
        place(inputs[layer + 1], first[layer + 1] + row, values, 2 ** (layer + 1))

    def finish_and_conv(layer, order, norm):
        carry = (jnp.zeros((channels, 128), f32),) * 2
        step = 2 ** (layer + 1)
        ready, waiting = set(), list(range(rows))
        for row in order:
            finish_row(layer, row, norm)
            ready.add(row)
            for out in list(waiting):
                if {out - step, out, out + step} <= ready:
                    carry = own_row(layer + 1, out, carry)
                    waiting.remove(out)
        assert not waiting
        return carry

    nothing = (jnp.zeros((channels, 128), f32),) * 2

    with scope("b0_conv0_inner"):
        carry = nothing
        for row in range(1, rows - 1):
            carry = own_row(0, row, carry)
        send_edge(2)
    with scope("b1_far"):
        for n in range(len(far)):
            far_wait(n)
            if n + 1 < len(far):
                far_signal(n + 1)
    with scope("b2_take0"):
        take_edge(0)
    with scope("b3_conv0_edge"):
        place_shifts(REACH - 1)
        place_shifts(REACH + rows)
        for row in (0, rows - 1):
            carry = own_row(0, row, carry)
    with scope("b4_tally0"):
        tally(0, carry)
        send_tally(0)
    with scope("b5_send"):
        send_edge(3)
        set_taps(1)
        set_taps(2)
        fetches["gain"].wait()
        fetches["bias"].wait()
    with scope("b6_take12"):
        take_edge(REACH)
        take_edge(1)
        take_edge(2)
    with scope("b7_halo0"):
        masks[1] = widen(flag_in[0])
        masks[2] = widen(flag_in[1])
        for piece in (1, 2):
            place_shifts(REACH - 1 - piece)
            place_shifts(REACH + rows + piece)
        for row in (-1, rows, -2, rows + 1):
            put(row, conv_row(0, row))
    with scope("b8_send4"):
        sent_edge(3)
        send_edge(4)
    with scope("c0_take_tally0"):
        norm0 = take_tally(0)
    with scope("c1_layer1"):
        order = (0, 2, 4, 1, 3, 5, -2, -1, 6, 7, rows, rows + 1)
        carry = finish_and_conv(0, order, norm0)
    with scope("c2_tally1"):
        tally(1, carry)
        send_tally(1)
    with scope("c3_send"):
        sent_edge(4)
        send_edge(5)
        send_edge(6)
    for piece in range(3, REACH):
        with scope(f"d{piece}_take"):
            take_edge(piece)
        with scope(f"d{piece}_work"):
            place_shifts(REACH - 1 - piece)
            place_shifts(REACH + rows + piece)
            for row in (-piece, rows - 1 + piece):
                put(row, conv_row(0, row))
            for row in (-piece, rows - 1 + piece):
                finish_row(0, row, norm0)
            near_row = piece - 2
            for row in (-near_row, rows - 1 + near_row):
                put(row, conv_row(1, row))
    with scope("e0_take_tally1"):
        norm1 = take_tally(1)
    with scope("e1_layer2"):
        order = (-4, 0, 4, 8, -3, 1, 5, 9, -2, 2, 6, 10, -1, 3, 7, 11)
        carry = finish_and_conv(1, order, norm1)
    with scope("e2_tally2"):
        tally(2, carry)
        send_tally(2)
    with scope("e3_sent"):
        for piece in range(REACH + 1):
            if piece not in (3, 4):
                sent_edge(piece)
        for layer in range(LAYERS - 1):

            def one(step, carry):
                tally_copy(layer, step, lax.rem(me + step, peers), me).wait_send()
                return carry

            lax.fori_loop(1, peers, one, 0)
    with scope("f0_take_tally2"):
        norm2 = take_tally(2)
    with scope("f1_norm"):
        for n in range(3):
            norm_ref[n] = jnp.broadcast_to(norm2[n], (channels, 128))

        def last(step, carry):
            tally_copy(LAYERS - 1, step, lax.rem(me + step, peers), me).wait_send()
            return carry

        lax.fori_loop(1, peers, last, 0)


def finish(own_ref, norm_ref, mask_ref, out_ref, result, turned, sems):
    channels, rows, cols = out_ref.shape
    copies = []
    for at in range(cols // 128):
        here = slice(at * 128, (at + 1) * 128)
        for row in range(rows):
            scaled = (own_ref[row, :, here] - norm_ref[0]) * norm_ref[1] + norm_ref[2]
            turned[at, pl.ds(row, channels, stride=rows), :] = (
                jnp.maximum(scaled, 0.0) * mask_ref[0:1, here]
            )
        result[at] = turned[at].reshape(channels, rows, 128).astype(result.dtype)
        copy = pltpu.make_async_copy(result.at[at], out_ref.at[:, :, here], sems.at[at])
        copy.start()
        copies.append(copy)
    for copy in copies:
        copy.wait()


def per_device(peers, *arrays):
    channels, rows, cols = arrays[0].shape
    assert rows == TILE and rows > REACH and arrays[1].shape[0] == 1 and channels < 128
    f32, bf16 = jnp.float32, jnp.bfloat16
    vmem = pl.BlockSpec(memory_space=pltpu.VMEM)
    hbm = pl.BlockSpec(memory_space=pltpu.HBM)
    own, norm, mask = pl.pallas_call(
        functools.partial(stack, peers),
        out_shape=(
            jax.ShapeDtypeStruct((rows, channels, cols), f32),
            jax.ShapeDtypeStruct((3, channels, 128), f32),
            jax.ShapeDtypeStruct((8, cols), f32),
        ),
        in_specs=[hbm] * 7,
        out_specs=(vmem,) * 3,
        scratch_shapes=[
            pltpu.VMEM((channels, rows, cols), bf16),
            pltpu.VMEM(arrays[1].shape, jnp.int32),
            pltpu.VMEM(arrays[2].shape, jnp.int32),
            pltpu.VMEM(arrays[3].shape, f32),
            pltpu.VMEM(arrays[5].shape, f32),
            pltpu.VMEM(arrays[6].shape, f32),
            pltpu.VMEM(arrays[4].shape, bf16),
            pltpu.VMEM((cols // 128, channels * rows, 128), f32),
            pltpu.VMEM((channels, cols), f32),
            pltpu.VMEM((3, rows + 2 * REACH, channels, cols), bf16),
            pltpu.VMEM((3, rows + 2 * (REACH - 1), channels, cols), bf16),
            pltpu.VMEM((3, rows + 2 * (REACH - 3), channels, cols), bf16),
            pltpu.VMEM((2 * (REACH - 1), channels, cols), f32),
            pltpu.VMEM((LAYERS, channels, 9 * channels), bf16),
            pltpu.VMEM((3, 8, cols), f32),
            pltpu.VMEM((8, 128), f32),
            pltpu.VMEM((2, 8, 128), f32),
            pltpu.VMEM((LAYERS, 2, 128), f32),
            pltpu.VMEM((LAYERS, peers, 2, 128), f32),
            pltpu.SemaphoreType.DMA((REACH + 1, 2)),
            pltpu.SemaphoreType.DMA((REACH + 1, 2)),
            pltpu.SemaphoreType.DMA((LAYERS, peers)),
            pltpu.SemaphoreType.DMA((LAYERS, peers)),
            pltpu.SemaphoreType.DMA((7,)),
            pltpu.SemaphoreType.REGULAR((max(len(rounds(peers)), 1), 2)),
        ],
        compiler_params=pltpu.CompilerParams(
            collective_id=0, has_side_effects=True, vmem_limit_bytes=44 * 2**20
        ),
    )(*(pltpu.with_memory_space_constraint(array, pltpu.HBM) for array in arrays))
    return pl.pallas_call(
        finish,
        out_shape=jax.ShapeDtypeStruct((channels, rows, cols), bf16),
        in_specs=[vmem] * 3,
        out_specs=pl.BlockSpec(memory_space=pl.ANY),
        scratch_shapes=[
            pltpu.VMEM((cols // 128, channels, rows, 128), bf16),
            pltpu.VMEM((cols // 128, channels * rows, 128), f32),
            pltpu.SemaphoreType.DMA((cols // 128,)),
        ],
        compiler_params=pltpu.CompilerParams(vmem_limit_bytes=8 * 2**20),
    )(own, norm, mask)


def solution(mesh):
    banded = P(None, ("groups", "rows"), None)
    tiled = P(("groups", "rows"), None)
    return jax.shard_map(
        functools.partial(per_device, mesh.shape["rows"]),
        mesh=mesh,
        in_specs=(banded, tiled, tiled, P(), P(), P(), P()),
        out_specs=banded,
        check_vma=False,
    )
```

```python
import functools

import jax
import jax.numpy as jnp
from jax import lax
from jax.experimental import pallas as pl
from jax.experimental.pallas import tpu as pltpu
from jax.sharding import PartitionSpec as P

LAYERS = 3
TILE = 8
STAINS = 4
REACH = 2**LAYERS - 1
EPSILON = 1e-05
NEAR = 4
MESH = pl.DeviceIdType.MESH
scope = jax.named_scope


def rounds(peers):
    out = []
    reach = NEAR
    while reach < peers - 1:
        out.append(reach)
        reach *= 2
    return tuple(out)


def stack(
    peers,
    slide_ref,
    flags_ref,
    index_ref,
    stain_ref,
    weights_ref,
    gain_ref,
    bias_ref,
    own_ref,
    norm_ref,
    mask_ref,
    slide,
    flags,
    index,
    stain,
    gains,
    biases,
    weights,
    turned,
    scale,
    x0,
    x1,
    x2,
    response,
    taps,
    masks,
    flag_out,
    flag_in,
    tally_out,
    tally_in,
    edge_send,
    edge_recv,
    tally_send,
    tally_recv,
    local_sem,
    far_sem,
):
    channels, rows, cols = slide_ref.shape
    tiles = flags_ref.shape[1]
    bf16, f32 = jnp.bfloat16, jnp.float32
    me = lax.axis_index("rows")
    odd = lax.rem(me, 2)
    turn = 1 - 2 * odd
    partner = (me - turn, me + turn)
    exists = tuple((there >= 0) & (there < peers) for there in partner)
    phase = lax.rem(me, 4)
    through = (phase == 0) | (phase == 3)
    inputs = (x0, x1, x2)
    first = (REACH, REACH - 1, REACH - 3)
    base = REACH - 1
    chunks = cols // 128
    barrier = pltpu.get_barrier_semaphore()

    fetches = {}
    for n, (name, source, target) in enumerate(
        (
            ("flags", flags_ref, flags),
            ("index", index_ref, index),
            ("stain", stain_ref, stain),
            ("slide", slide_ref, slide),
            ("weights", weights_ref, weights),
            ("gain", gain_ref, gains),
            ("bias", bias_ref, biases),
        )
    ):
        fetches[name] = pltpu.make_async_copy(source, target, local_sem.at[n])
        fetches[name].start()

    flag_in[...] = jnp.zeros_like(flag_in)

    def at_distance(distance, side):
        there = me - distance if side == 0 else me + distance
        return there, there >= 0 if side == 0 else there < peers

    for distance in range(1, NEAR + 1):
        for side in range(2):
            there, is_there = at_distance(distance, side)

            @pl.when(is_there)
            def _():
                pl.semaphore_signal(barrier, inc=1, device_id={"rows": there}, device_id_type=MESH)

    far = rounds(peers)

    def far_signal(n):
        for side in range(2):
            there, is_there = at_distance(far[n], side)

            @pl.when(is_there)
            def _():
                pl.semaphore_signal(
                    far_sem.at[n, 1 - side], inc=1, device_id={"rows": there}, device_id_type=MESH
                )

    def far_wait(n):
        for side in range(2):
            _, is_there = at_distance(far[n], side)

            @pl.when(is_there)
            def _():
                pl.semaphore_wait(far_sem.at[n, side], 1)

    spread = (
        lax.broadcasted_iota(jnp.int32, (128, cols), 1) // TILE
        == lax.broadcasted_iota(jnp.int32, (128, cols), 0)
    ).astype(f32)
    eye = lax.broadcasted_iota(jnp.int32, (channels, channels), 0) == lax.broadcasted_iota(
        jnp.int32, (channels, channels), 1
    )

    def column(row):
        return jnp.sum(jnp.where(eye, row, 0.0), axis=1, keepdims=True)

    def as_row(col):
        return jnp.sum(jnp.where(eye, col, 0.0), axis=0, keepdims=True)

    def widen(values):
        return jnp.dot(values, spread, preferred_element_type=f32)

    flag_out[...] = jnp.zeros_like(flag_out)

    with scope("a0_small"):
        fetches["flags"].wait()
        fetches["index"].wait()
        fetches["stain"].wait()
    with scope("a1_scale"):
        flag_out[:, 0:tiles] = jnp.broadcast_to(
            flags[...].astype(f32), (flag_out.shape[0], tiles)
        )
        masks[0] = widen(flag_out[...])
        mask_ref[...] = masks[0]
        classes = jnp.dot(
            jnp.broadcast_to(index[...].astype(f32), (8, tiles)),
            spread[0:tiles],
            preferred_element_type=f32,
        )[0:1]
        factor = jnp.zeros((channels, cols), f32)
        for kind in range(STAINS):
            factor = jnp.where(classes == kind, column(stain[kind : kind + 1, :]), factor)
        scale[...] = factor * masks[0, 0:1, :]
    with scope("a2_slide"):
        fetches["slide"].wait()
    with scope("a3_turn"):
        for at in range(chunks):
            turned[at] = (
                slide[:, :, at * 128 : (at + 1) * 128].astype(f32).reshape(channels * rows, 128)
            )

    lane = lax.broadcasted_iota(jnp.int32, (1, 128), 1)

    def shifts(values, spacing):
        inside = (lane >= spacing).astype(f32).astype(bf16)
        left = pltpu.roll(values, spacing, 1)
        left = jnp.concatenate([left[:, 0:128] * inside, left[:, 128:]], axis=1)
        inside = (lane < 128 - spacing).astype(f32).astype(bf16)
        right = pltpu.roll(values, cols - spacing, 1)
        right = jnp.concatenate([right[:, : cols - 128], right[:, cols - 128 :] * inside], axis=1)
        return left, right

    def place(buffer, row, values, spacing):
        buffer[1, row] = values
        buffer[0, row], buffer[2, row] = shifts(values, spacing)

    def true_row(row):
        return odd * (rows - 1) + turn * row

    def load_row(row):
        values = jnp.concatenate(
            [
                turned[at, pl.ds(true_row(row), channels, stride=rows), :]
                for at in range(chunks)
            ],
            axis=1,
        )
        place(x0, first[0] + row, (values * scale[...]).astype(bf16), 1)

    def edge_copy(piece, side):
        if piece == REACH:
            source, target = flag_out, flag_in.at[side]
        else:
            start = REACH + piece if side == 0 else REACH + rows - 1 - piece
            land = REACH - 1 - piece if side == 0 else REACH + rows + piece
            source, target = x0.at[1, start], x0.at[1, land]
        return pltpu.make_async_remote_copy(
            src_ref=source,
            dst_ref=target,
            send_sem=edge_send.at[piece, side],
            recv_sem=edge_recv.at[piece, side],
            device_id={"rows": partner[side]},
            device_id_type=MESH,
        )

    def send_edges(side, pieces, which=None):
        @pl.when(exists[side] if which is None else exists[side] & which)
        def _():
            for piece in pieces:
                edge_copy(piece, side).start()

    def take_edges(side, pieces):
        @pl.when(exists[side])
        def _():
            for piece in pieces:
                edge_copy(piece, side).wait_recv()

    direct = jnp.logical_not(through)

    with scope("a4_edge_rows"):
        load_row(0)
        load_row(rows - 1)
    with scope("a5_barrier"):
        near = jnp.minimum(me, NEAR) + jnp.minimum(peers - 1 - me, NEAR)
        pl.semaphore_wait(barrier, near)
    with scope("a6_send"):
        send_edges(0, (0, REACH))
        send_edges(1, (0, REACH))
        if far:
            far_signal(0)
    with scope("a7_rows"):
        for row in range(1, rows - 1):
            load_row(row)
        send_edges(0, (1,), direct)
        send_edges(1, range(1, REACH))

        @pl.when(jnp.logical_not(exists[0]))
        def _():
            x0[1, 0:REACH] = jnp.zeros((REACH, channels, cols), bf16)

        @pl.when(jnp.logical_not(exists[1]))
        def _():
            x0[1, REACH + rows : 2 * REACH + rows] = jnp.zeros((REACH, channels, cols), bf16)

    def set_taps(layer):
        for a in range(3):
            for b in range(3):
                tap = 3 * a + b
                taps[layer, :, tap * channels : (tap + 1) * channels] = weights[
                    layer, 3 * (1 + turn * (a - 1)) + b
                ]

    with scope("a8_taps"):
        fetches["weights"].wait()
        set_taps(0)

    def place_shifts(row):
        at = first[0] + row
        x0[0, at], x0[2, at] = shifts(x0[1, at], 1)

    def conv_row(layer, row):
        spacing = 2**layer
        source = inputs[layer]
        window = jnp.concatenate(
            [
                source[b, first[layer] + row + (a - 1) * spacing]
                for a in range(3)
                for b in range(3)
            ],
            axis=0,
        )
        return jnp.dot(taps[layer], window, preferred_element_type=f32)

    def halo_row(layer, row):
        response[base + row] = conv_row(layer, row)

    def fold(values):
        total = values[:, 0:128]
        for at in range(128, cols, 128):
            total = total + values[:, at : at + 128]
        return total

    def own_row(layer, row, carry):
        sums, squares = carry
        own = conv_row(layer, row)
        if layer < LAYERS - 1:
            response[base + row] = own
        else:
            own_ref[true_row(row)] = own
        masked = own * masks[0, 0:1, :]
        return sums + fold(masked), squares + fold(masked * own)

    def tally(layer, carry):
        sums, squares = carry
        tally_out[layer, 0:1, 0:channels] = as_row(jnp.sum(sums, axis=1, keepdims=True))
        tally_out[layer, 1:2, 0:channels] = as_row(jnp.sum(squares, axis=1, keepdims=True))
        pixels = jnp.sum(masks[0, 0:1, :], axis=1, keepdims=True) * rows
        tally_out[layer, :, channels:] = jnp.broadcast_to(pixels, (2, 128 - channels))
        tally_in[layer, peers - 1] = tally_out[layer]

    def send_tally(layer):
        order = sorted(range(1, peers), key=lambda step: abs(step - peers // 2))
        for step in order:
            pltpu.make_async_remote_copy(
                src_ref=tally_out.at[layer],
                dst_ref=tally_in.at[layer, peers - 1 - step],
                send_sem=tally_send.at[layer],
                recv_sem=tally_recv.at[layer],
                device_id={"rows": lax.rem(me + step, peers)},
                device_id_type=MESH,
            ).start()

    def all_tallies(layer, sem):
        others = tally_in.at[layer, 0 : peers - 1]
        return pltpu.make_async_copy(others, others, sem.at[layer])

    def take_tally(layer):
        all_tallies(layer, tally_recv).wait()
        total = jnp.sum(tally_in[layer], axis=0)
        count = total[0:1, channels : channels + 1]
        average = total[0:1, 0:channels] / count
        variance = jnp.maximum(total[1:2, 0:channels] / count - average * average, 0.0)
        factor = gains[layer : layer + 1, :] * lax.rsqrt(variance + EPSILON)
        return column(average), column(factor), column(biases[layer : layer + 1, :])

    def finish_row(layer, row, norm):
        average, factor, bias = norm
        which = 0 if 0 <= row < rows else 1 if row < 0 else 2
        scaled = ((response[base + row] - average) * factor + bias).astype(bf16)
        mask = masks[which, 0:1, :].astype(bf16)
        values = jnp.maximum(scaled, jnp.zeros((), bf16)) * mask
        place(inputs[layer + 1], first[layer + 1] + row, values, 2 ** (layer + 1))

    def finish_and_conv(layer, order, norm, carry, ready, waiting):
        step = 2 ** (layer + 1)
        for row in order:
            finish_row(layer, row, norm)
            ready.add(row)
            for out in list(waiting):
                if {out - step, out, out + step} <= ready:
                    carry = own_row(layer + 1, out, carry)
                    waiting.remove(out)
        return carry

    nothing = (jnp.zeros((channels, 128), f32),) * 2

    with scope("b0_conv0_inner"):
        carry = nothing
        for row in range(1, rows - 1):
            carry = own_row(0, row, carry)
        set_taps(1)
        set_taps(2)
        send_edges(0, (1,), through)
    with scope("b1_far"):
        for n in range(len(far) - 1):
            far_wait(n)
            far_signal(n + 1)
    with scope("b2_fast0"):
        take_edges(1, (0,))
        place_shifts(rows)
        carry = own_row(0, rows - 1, carry)
    with scope("b3_take0"):
        take_edges(0, (0,))
    with scope("b4_slow0"):
        place_shifts(-1)
        carry = own_row(0, 0, carry)
    with scope("b5_far"):
        if far:
            far_wait(len(far) - 1)
    with scope("b6_tally0"):
        tally(0, carry)
        send_tally(0)
        send_edges(0, (2, 3), direct)
        send_edges(0, (2,), through)
    with scope("b7_fast12"):
        fetches["gain"].wait()
        fetches["bias"].wait()
        take_edges(1, (REACH, *range(1, REACH)))
        masks[2] = widen(flag_in[1])
        for piece in range(1, REACH):
            place_shifts(rows + piece)
        for piece in range(1, REACH):
            halo_row(0, rows - 1 + piece)
    with scope("b8_take1"):
        take_edges(0, (REACH, 1))
    with scope("b8_slow1"):
        masks[1] = widen(flag_in[0])
        place_shifts(-2)
        halo_row(0, -1)
        send_edges(0, (3,), through)
    with scope("b9_take2"):
        take_edges(0, (2,))
    with scope("b9_slow2"):
        place_shifts(-3)
        halo_row(0, -2)
        send_edges(0, (4,))
    with scope("c0_take_tally0"):
        norm0 = take_tally(0)
    with scope("c1_layer1"):
        order = (3, 5, 7, 2, 4, 6, rows, rows + 1, 1, 0, -1, -2)
        carry = finish_and_conv(0, order, norm0, nothing, set(), list(range(rows)))
    with scope("c2_tally1"):
        tally(1, carry)
        send_tally(1)
        send_edges(0, (5, 6), direct)
        send_edges(0, (5,), through)
    with scope("d0_fast"):
        for piece in range(3, REACH):
            finish_row(0, rows - 1 + piece, norm0)
        for piece in range(3, REACH):
            halo_row(1, rows - 3 + piece)
        send_edges(0, (6,), through)

    def slow_piece(piece):
        with scope(f"d{piece}_take"):
            take_edges(0, (piece,))
        with scope(f"d{piece}_work"):
            place_shifts(-piece - 1)
            halo_row(0, -piece)
            finish_row(0, -piece, norm0)
            halo_row(1, 2 - piece)

    slow_piece(3)
    slow_piece(4)
    slow_piece(5)
    with scope("e0_take_tally1"):
        norm1 = take_tally(1)
    ready, waiting = set(), list(range(rows))
    with scope("e1_layer2"):
        order = (11, 7, 3, 10, 6, 2, -2, 9, 5, 1, -3, 8, 4, 0, -1)
        carry = finish_and_conv(1, order, norm1, nothing, ready, waiting)
    slow_piece(6)
    with scope("e6_layer2"):
        carry = finish_and_conv(1, (-4,), norm1, carry, ready, waiting)
    assert not waiting
    with scope("e7_tally2"):
        tally(2, carry)
        send_tally(2)
    with scope("e8_sent"):
        for side in range(2):

            @pl.when(exists[side])
            def _():
                for piece in range(REACH + 1):
                    edge_copy(piece, side).wait_send()

        for layer in range(LAYERS):
            all_tallies(layer, tally_send).wait()
    with scope("f0_take_tally2"):
        norm2 = take_tally(2)
    with scope("f1_norm"):
        for n in range(3):
            norm_ref[n] = jnp.broadcast_to(norm2[n], (channels, 128))


def finish(own_ref, norm_ref, mask_ref, out_ref, result, turned, sems):
    channels, rows, cols = out_ref.shape
    copies = []
    for at in range(cols // 128):
        here = slice(at * 128, (at + 1) * 128)
        for row in range(rows):
            scaled = (own_ref[row, :, here] - norm_ref[0]) * norm_ref[1] + norm_ref[2]
            turned[at, pl.ds(row, channels, stride=rows), :] = (
                jnp.maximum(scaled, 0.0) * mask_ref[0:1, here]
            )
        result[at] = turned[at].reshape(channels, rows, 128).astype(result.dtype)
        copy = pltpu.make_async_copy(result.at[at], out_ref.at[:, :, here], sems.at[at])
        copy.start()
        copies.append(copy)
    for copy in copies:
        copy.wait()


def per_device(peers, *arrays):
    channels, rows, cols = arrays[0].shape
    assert rows == TILE and rows > REACH and arrays[1].shape[0] == 1 and channels < 128
    f32, bf16 = jnp.float32, jnp.bfloat16
    vmem = pl.BlockSpec(memory_space=pltpu.VMEM)
    hbm = pl.BlockSpec(memory_space=pltpu.HBM)
    own, norm, mask = pl.pallas_call(
        functools.partial(stack, peers),
        out_shape=(
            jax.ShapeDtypeStruct((rows, channels, cols), f32),
            jax.ShapeDtypeStruct((3, channels, 128), f32),
            jax.ShapeDtypeStruct((8, cols), f32),
        ),
        in_specs=[hbm] * 7,
        out_specs=(vmem,) * 3,
        scratch_shapes=[
            pltpu.VMEM((channels, rows, cols), bf16),
            pltpu.VMEM(arrays[1].shape, jnp.int32),
            pltpu.VMEM(arrays[2].shape, jnp.int32),
            pltpu.VMEM(arrays[3].shape, f32),
            pltpu.VMEM(arrays[5].shape, f32),
            pltpu.VMEM(arrays[6].shape, f32),
            pltpu.VMEM(arrays[4].shape, bf16),
            pltpu.VMEM((cols // 128, channels * rows, 128), f32),
            pltpu.VMEM((channels, cols), f32),
            pltpu.VMEM((3, rows + 2 * REACH, channels, cols), bf16),
            pltpu.VMEM((3, rows + 2 * (REACH - 1), channels, cols), bf16),
            pltpu.VMEM((3, rows + 2 * (REACH - 3), channels, cols), bf16),
            pltpu.VMEM((rows + 2 * (REACH - 1), channels, cols), f32),
            pltpu.VMEM((LAYERS, channels, 9 * channels), bf16),
            pltpu.VMEM((3, 8, cols), f32),
            pltpu.VMEM((8, 128), f32),
            pltpu.VMEM((2, 8, 128), f32),
            pltpu.VMEM((LAYERS, 2, 128), f32),
            pltpu.VMEM((LAYERS, peers, 2, 128), f32),
            pltpu.SemaphoreType.DMA((REACH + 1, 2)),
            pltpu.SemaphoreType.DMA((REACH + 1, 2)),
            pltpu.SemaphoreType.DMA((LAYERS,)),
            pltpu.SemaphoreType.DMA((LAYERS,)),
            pltpu.SemaphoreType.DMA((7,)),
            pltpu.SemaphoreType.REGULAR((max(len(rounds(peers)), 1), 2)),
        ],
        compiler_params=pltpu.CompilerParams(
            collective_id=0, has_side_effects=True, vmem_limit_bytes=44 * 2**20
        ),
    )(*(pltpu.with_memory_space_constraint(array, pltpu.HBM) for array in arrays))
    return pl.pallas_call(
        finish,
        out_shape=jax.ShapeDtypeStruct((channels, rows, cols), bf16),
        in_specs=[vmem] * 3,
        out_specs=pl.BlockSpec(memory_space=pl.ANY),
        scratch_shapes=[
            pltpu.VMEM((cols // 128, channels, rows, 128), bf16),
            pltpu.VMEM((cols // 128, channels * rows, 128), f32),
            pltpu.SemaphoreType.DMA((cols // 128,)),
        ],
        compiler_params=pltpu.CompilerParams(vmem_limit_bytes=8 * 2**20),
    )(own, norm, mask)


def solution(mesh):
    banded = P(None, ("groups", "rows"), None)
    tiled = P(("groups", "rows"), None)
    return jax.shard_map(
        functools.partial(per_device, mesh.shape["rows"]),
        mesh=mesh,
        in_specs=(banded, tiled, tiled, P(), P(), P(), P()),
        out_specs=banded,
        check_vma=False,
    )
```

```python
import functools

import jax
import jax.numpy as jnp
from jax import lax
from jax.experimental import pallas as pl
from jax.experimental.pallas import tpu as pltpu
from jax.sharding import PartitionSpec as P

LAYERS = 3
TILE = 8
STAINS = 4
REACH = 2**LAYERS - 1
EPSILON = 1e-05
NEAR = 4
MESH = pl.DeviceIdType.MESH
scope = jax.named_scope


def rounds(peers):
    out = []
    reach = NEAR
    while reach < peers - 1:
        out.append(reach)
        reach *= 2
    return tuple(out)


def stack(
    peers,
    slide_ref,
    flags_ref,
    index_ref,
    stain_ref,
    weights_ref,
    gain_ref,
    bias_ref,
    own_ref,
    norm_ref,
    mask_ref,
    slide,
    flags,
    index,
    stain,
    gains,
    biases,
    weights,
    turned,
    scale,
    x0,
    x1,
    x2,
    response,
    taps,
    masks,
    flag_out,
    flag_in,
    tally_out,
    tally_in,
    edge_send,
    edge_recv,
    tally_send,
    tally_recv,
    local_sem,
    far_sem,
):
    channels, rows, cols = slide_ref.shape
    tiles = flags_ref.shape[1]
    bf16, f32 = jnp.bfloat16, jnp.float32
    me = lax.axis_index("rows")
    odd = lax.rem(me, 2)
    turn = 1 - 2 * odd
    partner = (me - turn, me + turn)
    exists = tuple((there >= 0) & (there < peers) for there in partner)
    phase = lax.rem(me, 4)
    through = (phase == 0) | (phase == 3)
    inputs = (x0, x1, x2)
    first = (REACH, REACH - 1, REACH - 3)
    base = REACH - 1
    chunks = cols // 128
    barrier = pltpu.get_barrier_semaphore()

    fetches = {}
    for n, (name, source, target) in enumerate(
        (
            ("flags", flags_ref, flags),
            ("index", index_ref, index),
            ("stain", stain_ref, stain),
            ("slide", slide_ref, slide),
            ("weights", weights_ref, weights),
            ("gain", gain_ref, gains),
            ("bias", bias_ref, biases),
        )
    ):
        fetches[name] = pltpu.make_async_copy(source, target, local_sem.at[n])
        fetches[name].start()

    flag_in[...] = jnp.zeros_like(flag_in)

    def at_distance(distance, side):
        there = me - distance if side == 0 else me + distance
        return there, there >= 0 if side == 0 else there < peers

    for distance in range(1, NEAR + 1):
        for side in range(2):
            there, is_there = at_distance(distance, side)

            @pl.when(is_there)
            def _():
                pl.semaphore_signal(barrier, inc=1, device_id={"rows": there}, device_id_type=MESH)

    far = rounds(peers)

    def far_signal(n):
        for side in range(2):
            there, is_there = at_distance(far[n], side)

            @pl.when(is_there)
            def _():
                pl.semaphore_signal(
                    far_sem.at[n, 1 - side], inc=1, device_id={"rows": there}, device_id_type=MESH
                )

    def far_wait(n):
        for side in range(2):
            _, is_there = at_distance(far[n], side)

            @pl.when(is_there)
            def _():
                pl.semaphore_wait(far_sem.at[n, side], 1)

    spread = (
        lax.broadcasted_iota(jnp.int32, (128, cols), 1) // TILE
        == lax.broadcasted_iota(jnp.int32, (128, cols), 0)
    ).astype(f32)
    eye = lax.broadcasted_iota(jnp.int32, (channels, channels), 0) == lax.broadcasted_iota(
        jnp.int32, (channels, channels), 1
    )

    def column(row):
        return jnp.sum(jnp.where(eye, row, 0.0), axis=1, keepdims=True)

    def as_row(col):
        return jnp.sum(jnp.where(eye, col, 0.0), axis=0, keepdims=True)

    def widen(values):
        return jnp.dot(values, spread, preferred_element_type=f32)

    flag_out[...] = jnp.zeros_like(flag_out)

    with scope("a0_small"):
        fetches["flags"].wait()
        fetches["index"].wait()
        fetches["stain"].wait()
    with scope("a1_scale"):
        flag_out[:, 0:tiles] = jnp.broadcast_to(
            flags[...].astype(f32), (flag_out.shape[0], tiles)
        )
        masks[0] = widen(flag_out[...])
        mask_ref[...] = masks[0]
        classes = jnp.dot(
            jnp.broadcast_to(index[...].astype(f32), (8, tiles)),
            spread[0:tiles],
            preferred_element_type=f32,
        )[0:1]
        factor = jnp.zeros((channels, cols), f32)
        for kind in range(STAINS):
            factor = jnp.where(classes == kind, column(stain[kind : kind + 1, :]), factor)
        scale[...] = factor * masks[0, 0:1, :]
    with scope("a2_slide"):
        fetches["slide"].wait()
    with scope("a3_turn"):
        for at in range(chunks):
            turned[at] = (
                slide[:, :, at * 128 : (at + 1) * 128].astype(f32).reshape(channels * rows, 128)
            )

    lane = lax.broadcasted_iota(jnp.int32, (1, 128), 1)

    def shifts(values, spacing):
        inside = (lane >= spacing).astype(f32).astype(bf16)
        left = pltpu.roll(values, spacing, 1)
        left = jnp.concatenate([left[:, 0:128] * inside, left[:, 128:]], axis=1)
        inside = (lane < 128 - spacing).astype(f32).astype(bf16)
        right = pltpu.roll(values, cols - spacing, 1)
        right = jnp.concatenate([right[:, : cols - 128], right[:, cols - 128 :] * inside], axis=1)
        return left, right

    def place(buffer, row, values, spacing):
        buffer[1, row] = values
        buffer[0, row], buffer[2, row] = shifts(values, spacing)

    def true_row(row):
        return odd * (rows - 1) + turn * row

    def load_row(row):
        values = jnp.concatenate(
            [
                turned[at, pl.ds(true_row(row), channels, stride=rows), :]
                for at in range(chunks)
            ],
            axis=1,
        )
        place(x0, first[0] + row, (values * scale[...]).astype(bf16), 1)

    def edge_copy(piece, side):
        if piece == REACH:
            source, target = flag_out, flag_in.at[side]
        else:
            start = REACH + piece if side == 0 else REACH + rows - 1 - piece
            land = REACH - 1 - piece if side == 0 else REACH + rows + piece
            source, target = x0.at[1, start], x0.at[1, land]
        return pltpu.make_async_remote_copy(
            src_ref=source,
            dst_ref=target,
            send_sem=edge_send.at[piece, side],
            recv_sem=edge_recv.at[piece, side],
            device_id={"rows": partner[side]},
            device_id_type=MESH,
        )

    def send_edges(side, pieces, which=None):
        @pl.when(exists[side] if which is None else exists[side] & which)
        def _():
            for piece in pieces:
                edge_copy(piece, side).start()

    def take_edges(side, pieces):
        @pl.when(exists[side])
        def _():
            for piece in pieces:
                edge_copy(piece, side).wait_recv()

    direct = jnp.logical_not(through)

    with scope("a4_edge_rows"):
        load_row(0)
        load_row(rows - 1)
    with scope("a5_barrier"):
        near = jnp.minimum(me, NEAR) + jnp.minimum(peers - 1 - me, NEAR)
        pl.semaphore_wait(barrier, near)
    with scope("a6_send"):
        send_edges(0, (0, REACH))
        send_edges(1, (0, REACH))
        if far:
            far_signal(0)
    with scope("a7_rows"):
        for row in range(1, rows - 1):
            load_row(row)
        send_edges(0, (1,), direct)
        send_edges(1, range(1, REACH))

        @pl.when(jnp.logical_not(exists[0]))
        def _():
            x0[1, 0:REACH] = jnp.zeros((REACH, channels, cols), bf16)

        @pl.when(jnp.logical_not(exists[1]))
        def _():
            x0[1, REACH + rows : 2 * REACH + rows] = jnp.zeros((REACH, channels, cols), bf16)

    def set_taps(layer):
        for a in range(3):
            for b in range(3):
                tap = 3 * a + b
                taps[layer, :, tap * channels : (tap + 1) * channels] = weights[
                    layer, 3 * (1 + turn * (a - 1)) + b
                ]

    with scope("a8_taps"):
        fetches["weights"].wait()
        set_taps(0)

    def place_shifts(row):
        at = first[0] + row
        x0[0, at], x0[2, at] = shifts(x0[1, at], 1)

    def conv_row(layer, row):
        spacing = 2**layer
        source = inputs[layer]
        window = jnp.concatenate(
            [
                source[b, first[layer] + row + (a - 1) * spacing]
                for a in range(3)
                for b in range(3)
            ],
            axis=0,
        )
        return jnp.dot(taps[layer], window, preferred_element_type=f32)

    def halo_row(layer, row):
        response[base + row] = conv_row(layer, row)

    def fold(values):
        total = values[:, 0:128]
        for at in range(128, cols, 128):
            total = total + values[:, at : at + 128]
        return total

    def own_row(layer, row, carry):
        sums, squares = carry
        own = conv_row(layer, row)
        if layer < LAYERS - 1:
            response[base + row] = own
        else:
            own_ref[true_row(row)] = own
        masked = own * masks[0, 0:1, :]
        return sums + fold(masked), squares + fold(masked * own)

    def tally(layer, carry):
        sums, squares = carry
        tally_out[layer, 0:1, 0:channels] = as_row(jnp.sum(sums, axis=1, keepdims=True))
        tally_out[layer, 1:2, 0:channels] = as_row(jnp.sum(squares, axis=1, keepdims=True))
        pixels = jnp.sum(masks[0, 0:1, :], axis=1, keepdims=True) * rows
        tally_out[layer, :, channels:] = jnp.broadcast_to(pixels, (2, 128 - channels))
        tally_in[layer, peers - 1] = tally_out[layer]

    def send_tally(layer):
        order = sorted(range(1, peers), key=lambda step: abs(step - peers // 2))
        for step in order:
            pltpu.make_async_remote_copy(
                src_ref=tally_out.at[layer],
                dst_ref=tally_in.at[layer, peers - 1 - step],
                send_sem=tally_send.at[layer],
                recv_sem=tally_recv.at[layer],
                device_id={"rows": lax.rem(me + step, peers)},
                device_id_type=MESH,
            ).start()

    def all_tallies(layer, sem):
        others = tally_in.at[layer, 0 : peers - 1]
        return pltpu.make_async_copy(others, others, sem.at[layer])

    def take_tally(layer):
        all_tallies(layer, tally_recv).wait()
        total = jnp.sum(tally_in[layer], axis=0)
        count = total[0:1, channels : channels + 1]
        average = total[0:1, 0:channels] / count
        variance = jnp.maximum(total[1:2, 0:channels] / count - average * average, 0.0)
        factor = gains[layer : layer + 1, :] * lax.rsqrt(variance + EPSILON)
        return column(average), column(factor), column(biases[layer : layer + 1, :])

    def finish_row(layer, row, norm):
        average, factor, bias = norm
        which = 0 if 0 <= row < rows else 1 if row < 0 else 2
        scaled = ((response[base + row] - average) * factor + bias).astype(bf16)
        mask = masks[which, 0:1, :].astype(bf16)
        values = jnp.maximum(scaled, jnp.zeros((), bf16)) * mask
        place(inputs[layer + 1], first[layer + 1] + row, values, 2 ** (layer + 1))

    def finish_and_conv(layer, order, norm, carry, ready, waiting):
        step = 2 ** (layer + 1)
        for row in order:
            finish_row(layer, row, norm)
            ready.add(row)
            for out in list(waiting):
                if {out - step, out, out + step} <= ready:
                    carry = own_row(layer + 1, out, carry)
                    waiting.remove(out)
        return carry

    nothing = (jnp.zeros((channels, 128), f32),) * 2

    with scope("b0_conv0_inner"):
        carry = nothing
        for row in range(1, rows - 1):
            carry = own_row(0, row, carry)
        set_taps(1)
        set_taps(2)
    with scope("b1_far"):
        for n in range(len(far) - 1):
            far_wait(n)
            far_signal(n + 1)
    with scope("b2_fast0"):
        take_edges(1, (0,))
        place_shifts(rows)
        carry = own_row(0, rows - 1, carry)
        send_edges(0, (1,), through)
    with scope("b3_take0"):
        take_edges(0, (0,))
    with scope("b4_slow0"):
        place_shifts(-1)
        carry = own_row(0, 0, carry)
    with scope("b5_far"):
        if far:
            far_wait(len(far) - 1)
    with scope("b6_tally0"):
        tally(0, carry)
        send_tally(0)
        send_edges(0, (2, 3), direct)
        send_edges(0, (2,), through)
    with scope("b7_fast12"):
        fetches["gain"].wait()
        fetches["bias"].wait()
        take_edges(1, (REACH, *range(1, REACH)))
        masks[2] = widen(flag_in[1])
        for piece in range(1, REACH):
            place_shifts(rows + piece)
        for piece in (1, 2):
            halo_row(0, rows - 1 + piece)
    with scope("b8_take1"):
        take_edges(0, (REACH, 1))
    with scope("b8_slow1"):
        masks[1] = widen(flag_in[0])
        place_shifts(-2)
        halo_row(0, -1)
    with scope("b8_fast"):
        for piece in range(3, REACH):
            halo_row(0, rows - 1 + piece)
        send_edges(0, (3,), through)
    with scope("b9_take2"):
        take_edges(0, (2,))
    with scope("b9_slow2"):
        place_shifts(-3)
        halo_row(0, -2)
        send_edges(0, (4,), through)
    with scope("c0_take_tally0"):
        norm0 = take_tally(0)
        send_edges(0, (5,), through)
    with scope("c1_layer1"):
        order = (3, 5, 7, 2, 4, 6, rows, rows + 1, 1, 0, -1, -2)
        carry = finish_and_conv(0, order, norm0, nothing, set(), list(range(rows)))
    with scope("c2_tally1"):
        tally(1, carry)
        send_tally(1)
        send_edges(0, (4, 5, 6), direct)
    with scope("d0_fast"):
        for piece in range(3, REACH):
            finish_row(0, rows - 1 + piece, norm0)
        for piece in range(3, REACH):
            halo_row(1, rows - 3 + piece)
        send_edges(0, (6,), through)

    def slow_pieces(pieces):
        with scope(f"d{pieces[0]}_take"):
            take_edges(0, pieces)
        with scope(f"d{pieces[0]}_work"):
            for piece in pieces:
                place_shifts(-piece - 1)
            for piece in pieces:
                halo_row(0, -piece)
            for piece in pieces:
                finish_row(0, -piece, norm0)
            for piece in pieces:
                halo_row(1, 2 - piece)

    def tail(before, after):
        for pieces in before:
            slow_pieces(pieces)
        with scope("e0_take_tally1"):
            norm1 = take_tally(1)
        ready, waiting = set(), list(range(rows))
        last = before[-1][-1]
        with scope("e1_layer2"):
            order = (11, 7, 3, 10, 6, 9, 5, 8, 4, 2, 1, 0) + tuple(range(-1, 1 - last, -1))
            carry = finish_and_conv(1, order, norm1, nothing, ready, waiting)
        for pieces in after:
            slow_pieces(pieces)
            with scope(f"e{pieces[0]}_layer2"):
                order = tuple(2 - piece for piece in pieces)
                carry = finish_and_conv(1, order, norm1, carry, ready, waiting)
        assert not waiting
        with scope("e7_tally2"):
            tally(2, carry)

    @pl.when(through)
    def _():
        tail(((3,), (4,)), ((5, 6),))

    @pl.when(direct)
    def _():
        tail(((3,),), ((4,), (5, 6)))

    with scope("e7_send"):
        send_tally(2)
    with scope("e8_sent"):
        for side in range(2):

            @pl.when(exists[side])
            def _():
                for piece in range(REACH + 1):
                    edge_copy(piece, side).wait_send()

        for layer in range(LAYERS):
            all_tallies(layer, tally_send).wait()
    with scope("f0_take_tally2"):
        norm2 = take_tally(2)
    with scope("f1_norm"):
        for n in range(3):
            norm_ref[n] = jnp.broadcast_to(norm2[n], (channels, 128))


def finish(own_ref, norm_ref, mask_ref, out_ref, result, turned, sems):
    channels, rows, cols = out_ref.shape
    copies = []
    for at in range(cols // 128):
        here = slice(at * 128, (at + 1) * 128)
        for row in range(rows):
            scaled = (own_ref[row, :, here] - norm_ref[0]) * norm_ref[1] + norm_ref[2]
            turned[at, pl.ds(row, channels, stride=rows), :] = (
                jnp.maximum(scaled, 0.0) * mask_ref[0:1, here]
            )
        result[at] = turned[at].reshape(channels, rows, 128).astype(result.dtype)
        copy = pltpu.make_async_copy(result.at[at], out_ref.at[:, :, here], sems.at[at])
        copy.start()
        copies.append(copy)
    for copy in copies:
        copy.wait()


def per_device(peers, *arrays):
    channels, rows, cols = arrays[0].shape
    assert rows == TILE and rows > REACH and arrays[1].shape[0] == 1 and channels < 128
    f32, bf16 = jnp.float32, jnp.bfloat16
    vmem = pl.BlockSpec(memory_space=pltpu.VMEM)
    hbm = pl.BlockSpec(memory_space=pltpu.HBM)
    own, norm, mask = pl.pallas_call(
        functools.partial(stack, peers),
        out_shape=(
            jax.ShapeDtypeStruct((rows, channels, cols), f32),
            jax.ShapeDtypeStruct((3, channels, 128), f32),
            jax.ShapeDtypeStruct((8, cols), f32),
        ),
        in_specs=[hbm] * 7,
        out_specs=(vmem,) * 3,
        scratch_shapes=[
            pltpu.VMEM((channels, rows, cols), bf16),
            pltpu.VMEM(arrays[1].shape, jnp.int32),
            pltpu.VMEM(arrays[2].shape, jnp.int32),
            pltpu.VMEM(arrays[3].shape, f32),
            pltpu.VMEM(arrays[5].shape, f32),
            pltpu.VMEM(arrays[6].shape, f32),
            pltpu.VMEM(arrays[4].shape, bf16),
            pltpu.VMEM((cols // 128, channels * rows, 128), f32),
            pltpu.VMEM((channels, cols), f32),
            pltpu.VMEM((3, rows + 2 * REACH, channels, cols), bf16),
            pltpu.VMEM((3, rows + 2 * (REACH - 1), channels, cols), bf16),
            pltpu.VMEM((3, rows + 2 * (REACH - 3), channels, cols), bf16),
            pltpu.VMEM((rows + 2 * (REACH - 1), channels, cols), f32),
            pltpu.VMEM((LAYERS, channels, 9 * channels), bf16),
            pltpu.VMEM((3, 8, cols), f32),
            pltpu.VMEM((8, 128), f32),
            pltpu.VMEM((2, 8, 128), f32),
            pltpu.VMEM((LAYERS, 2, 128), f32),
            pltpu.VMEM((LAYERS, peers, 2, 128), f32),
            pltpu.SemaphoreType.DMA((REACH + 1, 2)),
            pltpu.SemaphoreType.DMA((REACH + 1, 2)),
            pltpu.SemaphoreType.DMA((LAYERS,)),
            pltpu.SemaphoreType.DMA((LAYERS,)),
            pltpu.SemaphoreType.DMA((7,)),
            pltpu.SemaphoreType.REGULAR((max(len(rounds(peers)), 1), 2)),
        ],
        compiler_params=pltpu.CompilerParams(
            collective_id=0, has_side_effects=True, vmem_limit_bytes=44 * 2**20
        ),
    )(*(pltpu.with_memory_space_constraint(array, pltpu.HBM) for array in arrays))
    return pl.pallas_call(
        finish,
        out_shape=jax.ShapeDtypeStruct((channels, rows, cols), bf16),
        in_specs=[vmem] * 3,
        out_specs=pl.BlockSpec(memory_space=pl.ANY),
        scratch_shapes=[
            pltpu.VMEM((cols // 128, channels, rows, 128), bf16),
            pltpu.VMEM((cols // 128, channels * rows, 128), f32),
            pltpu.SemaphoreType.DMA((cols // 128,)),
        ],
        compiler_params=pltpu.CompilerParams(vmem_limit_bytes=8 * 2**20),
    )(own, norm, mask)


def solution(mesh):
    banded = P(None, ("groups", "rows"), None)
    tiled = P(("groups", "rows"), None)
    return jax.shard_map(
        functools.partial(per_device, mesh.shape["rows"]),
        mesh=mesh,
        in_specs=(banded, tiled, tiled, P(), P(), P(), P()),
        out_specs=banded,
        check_vma=False,
    )
```

```python
import functools

import jax
import jax.numpy as jnp
from jax import lax
from jax.experimental import pallas as pl
from jax.experimental.pallas import tpu as pltpu
from jax.sharding import PartitionSpec as P

LAYERS = 3
TILE = 8
STAINS = 4
REACH = 2**LAYERS - 1
EPSILON = 1e-05
NEAR = 4
LATE = 5
MESH = pl.DeviceIdType.MESH
scope = jax.named_scope


def rounds(peers):
    out = []
    reach = NEAR
    while reach < peers - 1:
        out.append(reach)
        reach *= 2
    return tuple(out)


def stack(
    peers,
    slide_ref,
    flags_ref,
    index_ref,
    stain_ref,
    weights_ref,
    gain_ref,
    bias_ref,
    own_ref,
    norm_ref,
    mask_ref,
    slide,
    flags,
    index,
    stain,
    gains,
    biases,
    weights,
    turned,
    scale,
    x0,
    x1,
    x2,
    response,
    late_out,
    late_in,
    taps,
    masks,
    flag_out,
    flag_in,
    tally_out,
    tally_in,
    edge_send,
    edge_recv,
    tally_send,
    tally_recv,
    local_sem,
    far_sem,
):
    channels, rows, cols = slide_ref.shape
    tiles = flags_ref.shape[1]
    bf16, f32 = jnp.bfloat16, jnp.float32
    me = lax.axis_index("rows")
    odd = lax.rem(me, 2)
    turn = 1 - 2 * odd
    partner = (me - turn, me + turn)
    exists = tuple((there >= 0) & (there < peers) for there in partner)
    phase = lax.rem(me, 4)
    through = (phase == 0) | (phase == 3)
    inputs = (x0, x1, x2)
    first = (REACH, REACH - 1, REACH - 3)
    base = REACH - 1
    chunks = cols // 128
    barrier = pltpu.get_barrier_semaphore()

    fetches = {}
    for n, (name, source, target) in enumerate(
        (
            ("flags", flags_ref, flags),
            ("index", index_ref, index),
            ("stain", stain_ref, stain),
            ("slide", slide_ref, slide),
            ("weights", weights_ref, weights),
            ("gain", gain_ref, gains),
            ("bias", bias_ref, biases),
        )
    ):
        fetches[name] = pltpu.make_async_copy(source, target, local_sem.at[n])
        fetches[name].start()

    flag_in[...] = jnp.zeros_like(flag_in)

    def at_distance(distance, side):
        there = me - distance if side == 0 else me + distance
        return there, there >= 0 if side == 0 else there < peers

    for distance in range(1, NEAR + 1):
        for side in range(2):
            there, is_there = at_distance(distance, side)

            @pl.when(is_there)
            def _():
                pl.semaphore_signal(barrier, inc=1, device_id={"rows": there}, device_id_type=MESH)

    far = rounds(peers)

    def far_signal(n):
        for side in range(2):
            there, is_there = at_distance(far[n], side)

            @pl.when(is_there)
            def _():
                pl.semaphore_signal(
                    far_sem.at[n, 1 - side], inc=1, device_id={"rows": there}, device_id_type=MESH
                )

    def far_wait(n):
        for side in range(2):
            _, is_there = at_distance(far[n], side)

            @pl.when(is_there)
            def _():
                pl.semaphore_wait(far_sem.at[n, side], 1)

    spread = (
        lax.broadcasted_iota(jnp.int32, (128, cols), 1) // TILE
        == lax.broadcasted_iota(jnp.int32, (128, cols), 0)
    ).astype(f32)
    eye = lax.broadcasted_iota(jnp.int32, (channels, channels), 0) == lax.broadcasted_iota(
        jnp.int32, (channels, channels), 1
    )

    def column(row):
        return jnp.sum(jnp.where(eye, row, 0.0), axis=1, keepdims=True)

    def as_row(col):
        return jnp.sum(jnp.where(eye, col, 0.0), axis=0, keepdims=True)

    def widen(values):
        return jnp.dot(values, spread, preferred_element_type=f32)

    flag_out[...] = jnp.zeros_like(flag_out)

    with scope("a0_small"):
        fetches["flags"].wait()
        fetches["index"].wait()
        fetches["stain"].wait()
    with scope("a1_scale"):
        flag_out[:, 0:tiles] = jnp.broadcast_to(
            flags[...].astype(f32), (flag_out.shape[0], tiles)
        )
        masks[0] = widen(flag_out[...])
        mask_ref[...] = masks[0]
        classes = jnp.dot(
            jnp.broadcast_to(index[...].astype(f32), (8, tiles)),
            spread[0:tiles],
            preferred_element_type=f32,
        )[0:1]
        factor = jnp.zeros((channels, cols), f32)
        for kind in range(STAINS):
            factor = jnp.where(classes == kind, column(stain[kind : kind + 1, :]), factor)
        scale[...] = factor * masks[0, 0:1, :]
    with scope("a2_slide"):
        fetches["slide"].wait()
    with scope("a3_turn"):
        for at in range(chunks):
            turned[at] = (
                slide[:, :, at * 128 : (at + 1) * 128].astype(f32).reshape(channels * rows, 128)
            )

    lane = lax.broadcasted_iota(jnp.int32, (1, 128), 1)

    def shifts(values, spacing):
        inside = (lane >= spacing).astype(f32).astype(bf16)
        left = pltpu.roll(values, spacing, 1)
        left = jnp.concatenate([left[:, 0:128] * inside, left[:, 128:]], axis=1)
        inside = (lane < 128 - spacing).astype(f32).astype(bf16)
        right = pltpu.roll(values, cols - spacing, 1)
        right = jnp.concatenate([right[:, : cols - 128], right[:, cols - 128 :] * inside], axis=1)
        return left, right

    def place(buffer, row, values, spacing):
        buffer[1, row] = values
        buffer[0, row], buffer[2, row] = shifts(values, spacing)

    def true_row(row):
        return odd * (rows - 1) + turn * row

    def load_row(row):
        values = jnp.concatenate(
            [
                turned[at, pl.ds(true_row(row), channels, stride=rows), :]
                for at in range(chunks)
            ],
            axis=1,
        )
        place(x0, first[0] + row, (values * scale[...]).astype(bf16), 1)

    def edge_copy(piece, side):
        if piece == REACH:
            source, target = flag_out, flag_in.at[side]
        elif side == 0 and piece >= LATE:
            source, target = late_out.at[piece - LATE], late_in.at[piece - LATE]
        else:
            start = REACH + piece if side == 0 else REACH + rows - 1 - piece
            land = REACH - 1 - piece if side == 0 else REACH + rows + piece
            source, target = x0.at[1, start], x0.at[1, land]
        return pltpu.make_async_remote_copy(
            src_ref=source,
            dst_ref=target,
            send_sem=edge_send.at[piece, side],
            recv_sem=edge_recv.at[piece, side],
            device_id={"rows": partner[side]},
            device_id_type=MESH,
        )

    def send_edges(side, pieces, which=None):
        @pl.when(exists[side] if which is None else exists[side] & which)
        def _():
            for piece in pieces:
                edge_copy(piece, side).start()

    def take_edges(side, pieces):
        @pl.when(exists[side])
        def _():
            for piece in pieces:
                edge_copy(piece, side).wait_recv()

    direct = jnp.logical_not(through)

    with scope("a4_edge_rows"):
        load_row(0)
        load_row(rows - 1)
    with scope("a5_barrier"):
        near = jnp.minimum(me, NEAR) + jnp.minimum(peers - 1 - me, NEAR)
        pl.semaphore_wait(barrier, near)
    with scope("a6_send"):
        send_edges(0, (0, REACH))
        send_edges(1, (0, REACH))
        if far:
            far_signal(0)
    with scope("a7_rows"):
        for row in range(1, rows - 1):
            load_row(row)
        send_edges(0, (1,), direct)
        send_edges(1, range(1, REACH))

        @pl.when(jnp.logical_not(exists[0]))
        def _():
            x0[1, 0:REACH] = jnp.zeros((REACH, channels, cols), bf16)
            late_in[...] = jnp.zeros_like(late_in)

        @pl.when(jnp.logical_not(exists[1]))
        def _():
            x0[1, REACH + rows : 2 * REACH + rows] = jnp.zeros((REACH, channels, cols), bf16)

    def set_taps(layer):
        for a in range(3):
            for b in range(3):
                tap = 3 * a + b
                taps[layer, :, tap * channels : (tap + 1) * channels] = weights[
                    layer, 3 * (1 + turn * (a - 1)) + b
                ]

    with scope("a8_taps"):
        fetches["weights"].wait()
        set_taps(0)

    def place_shifts(row):
        at = first[0] + row
        x0[0, at], x0[2, at] = shifts(x0[1, at], 1)

    def conv_row(layer, row):
        spacing = 2**layer
        source = inputs[layer]
        window = jnp.concatenate(
            [
                source[b, first[layer] + row + (a - 1) * spacing]
                for a in range(3)
                for b in range(3)
            ],
            axis=0,
        )
        return jnp.dot(taps[layer], window, preferred_element_type=f32)

    def halo_row(layer, row):
        response[base + row] = conv_row(layer, row)

    def fold(values):
        total = values[:, 0:128]
        for at in range(128, cols, 128):
            total = total + values[:, at : at + 128]
        return total

    def own_row(layer, row, carry):
        sums, squares = carry
        own = conv_row(layer, row)
        if layer < LAYERS - 1:
            response[base + row] = own
        else:
            own_ref[true_row(row)] = own
        masked = own * masks[0, 0:1, :]
        return sums + fold(masked), squares + fold(masked * own)

    def tally(layer, carry):
        sums, squares = carry
        tally_out[layer, 0:1, 0:channels] = as_row(jnp.sum(sums, axis=1, keepdims=True))
        tally_out[layer, 1:2, 0:channels] = as_row(jnp.sum(squares, axis=1, keepdims=True))
        pixels = jnp.sum(masks[0, 0:1, :], axis=1, keepdims=True) * rows
        tally_out[layer, :, channels:] = jnp.broadcast_to(pixels, (2, 128 - channels))
        tally_in[layer, peers - 1] = tally_out[layer]

    def send_tally(layer):
        order = sorted(range(1, peers), key=lambda step: abs(step - peers // 2))
        for step in order:
            pltpu.make_async_remote_copy(
                src_ref=tally_out.at[layer],
                dst_ref=tally_in.at[layer, peers - 1 - step],
                send_sem=tally_send.at[layer],
                recv_sem=tally_recv.at[layer],
                device_id={"rows": lax.rem(me + step, peers)},
                device_id_type=MESH,
            ).start()

    def all_tallies(layer, sem):
        others = tally_in.at[layer, 0 : peers - 1]
        return pltpu.make_async_copy(others, others, sem.at[layer])

    def take_tally(layer):
        all_tallies(layer, tally_recv).wait()
        total = jnp.sum(tally_in[layer], axis=0)
        count = total[0:1, channels : channels + 1]
        average = total[0:1, 0:channels] / count
        variance = jnp.maximum(total[1:2, 0:channels] / count - average * average, 0.0)
        factor = gains[layer : layer + 1, :] * lax.rsqrt(variance + EPSILON)
        return column(average), column(factor), column(biases[layer : layer + 1, :])

    def finish_row(layer, row, norm):
        average, factor, bias = norm
        which = 0 if 0 <= row < rows else 1 if row < 0 else 2
        scaled = ((response[base + row] - average) * factor + bias).astype(bf16)
        mask = masks[which, 0:1, :].astype(bf16)
        values = jnp.maximum(scaled, jnp.zeros((), bf16)) * mask
        place(inputs[layer + 1], first[layer + 1] + row, values, 2 ** (layer + 1))

    def finish_and_conv(layer, order, norm, carry, ready, waiting):
        step = 2 ** (layer + 1)
        for row in order:
            finish_row(layer, row, norm)
            ready.add(row)
            for out in list(waiting):
                if {out - step, out, out + step} <= ready:
                    carry = own_row(layer + 1, out, carry)
                    waiting.remove(out)
        return carry

    nothing = (jnp.zeros((channels, 128), f32),) * 2

    with scope("b0_conv0_inner"):
        carry = nothing
        for row in range(1, rows - 1):
            carry = own_row(0, row, carry)
        set_taps(1)
        set_taps(2)
    with scope("b1_far"):
        for n in range(len(far) - 1):
            far_wait(n)
            far_signal(n + 1)
    with scope("b2_fast0"):
        take_edges(1, (0,))
        place_shifts(rows)
        carry = own_row(0, rows - 1, carry)
        send_edges(0, (1,), through)
    with scope("b3_take0"):
        take_edges(0, (0,))
    with scope("b4_slow0"):
        place_shifts(-1)
        carry = own_row(0, 0, carry)
    with scope("b5_far"):
        if far:
            far_wait(len(far) - 1)
    with scope("b6_tally0"):
        tally(0, carry)
        send_tally(0)
        send_edges(0, (2, 3), direct)
        send_edges(0, (2,), through)
    with scope("b7_fast12"):
        fetches["gain"].wait()
        fetches["bias"].wait()
        take_edges(1, (REACH, *range(1, REACH)))
        masks[2] = widen(flag_in[1])
        for piece in range(1, REACH):
            place_shifts(rows + piece)
        for piece in (1, 2):
            halo_row(0, rows - 1 + piece)
    with scope("b8_take1"):
        take_edges(0, (REACH, 1))
    with scope("b8_slow1"):
        masks[1] = widen(flag_in[0])
        place_shifts(-2)
        halo_row(0, -1)
    with scope("b8_fast"):
        for piece in range(3, REACH):
            halo_row(0, rows - 1 + piece)
        send_edges(0, (3,), through)
    with scope("b9_take2"):
        take_edges(0, (2,))
    with scope("b9_slow2"):
        place_shifts(-3)
        halo_row(0, -2)
        send_edges(0, (4,))
    with scope("c0_take_tally0"):
        norm0 = take_tally(0)
    with scope("c1_layer1"):
        order = (3, 5, 7, 2, 4, 6, rows, rows + 1, 1, 0, -1, -2)
        carry = finish_and_conv(0, order, norm0, nothing, set(), list(range(rows)))
    with scope("c2_tally1"):
        tally(1, carry)
        send_tally(1)
    with scope("c3_late"):
        sums = jnp.sum(carry[0], axis=1, keepdims=True)
        pixels = jnp.sum(masks[0, 0:1, :], axis=1, keepdims=True) * rows
        centre = sums / pixels
        for piece in range(LATE, REACH):
            late_out[piece - LATE] = (response[base + piece - 3] - centre).astype(bf16)
            send_edges(0, (piece,), direct if piece > LATE else None)
    with scope("d0_fast"):
        for piece in range(3, REACH):
            finish_row(0, rows - 1 + piece, norm0)
        for piece in range(3, REACH):
            halo_row(1, rows - 3 + piece)

    def slow_piece(piece):
        with scope(f"d{piece}_take"):
            take_edges(0, (piece,))
        with scope(f"d{piece}_work"):
            place_shifts(-piece - 1)
            halo_row(0, -piece)
            finish_row(0, -piece, norm0)
            halo_row(1, 2 - piece)

    slow_piece(3)
    send_edges(0, range(LATE + 1, REACH), through)
    slow_piece(4)
    with scope("e0_take_tally1"):
        norm1 = take_tally(1)
    ready, waiting = set(), list(range(rows))
    with scope("e1_layer2"):
        order = (11, 7, 3, 10, 6, 9, 5, 8, 4, 2, 1, 0, -1, -2)
        carry = finish_and_conv(1, order, norm1, nothing, ready, waiting)
        theirs = tally_in[1, jnp.where(odd == 1, 0, peers - 2)]
        centre = column(theirs[0:1, 0:channels] / theirs[0:1, channels : channels + 1])
    with scope("e5_take"):
        take_edges(0, range(LATE, REACH))
    with scope("e6_late"):
        order = tuple(2 - piece for piece in range(LATE, REACH))
        for piece in range(LATE, REACH):
            response[base + 2 - piece] = late_in[piece - LATE].astype(f32) + centre
        carry = finish_and_conv(1, order, norm1, carry, ready, waiting)
    assert not waiting
    with scope("e7_tally2"):
        tally(2, carry)
    with scope("e7_send"):
        send_tally(2)
    with scope("e8_sent"):
        for side in range(2):

            @pl.when(exists[side])
            def _():
                for piece in range(REACH + 1):
                    edge_copy(piece, side).wait_send()

        for layer in range(LAYERS):
            all_tallies(layer, tally_send).wait()
    with scope("f0_take_tally2"):
        norm2 = take_tally(2)
    with scope("f1_norm"):
        for n in range(3):
            norm_ref[n] = jnp.broadcast_to(norm2[n], (channels, 128))


def finish(own_ref, norm_ref, mask_ref, out_ref, result, turned, sems):
    channels, rows, cols = out_ref.shape
    copies = []
    for at in range(cols // 128):
        here = slice(at * 128, (at + 1) * 128)
        for row in range(rows):
            scaled = (own_ref[row, :, here] - norm_ref[0]) * norm_ref[1] + norm_ref[2]
            turned[at, pl.ds(row, channels, stride=rows), :] = (
                jnp.maximum(scaled, 0.0) * mask_ref[0:1, here]
            )
        result[at] = turned[at].reshape(channels, rows, 128).astype(result.dtype)
        copy = pltpu.make_async_copy(result.at[at], out_ref.at[:, :, here], sems.at[at])
        copy.start()
        copies.append(copy)
    for copy in copies:
        copy.wait()


def per_device(peers, *arrays):
    channels, rows, cols = arrays[0].shape
    assert rows == TILE and rows > REACH and arrays[1].shape[0] == 1 and channels < 128
    f32, bf16 = jnp.float32, jnp.bfloat16
    vmem = pl.BlockSpec(memory_space=pltpu.VMEM)
    hbm = pl.BlockSpec(memory_space=pltpu.HBM)
    own, norm, mask = pl.pallas_call(
        functools.partial(stack, peers),
        out_shape=(
            jax.ShapeDtypeStruct((rows, channels, cols), f32),
            jax.ShapeDtypeStruct((3, channels, 128), f32),
            jax.ShapeDtypeStruct((8, cols), f32),
        ),
        in_specs=[hbm] * 7,
        out_specs=(vmem,) * 3,
        scratch_shapes=[
            pltpu.VMEM((channels, rows, cols), bf16),
            pltpu.VMEM(arrays[1].shape, jnp.int32),
            pltpu.VMEM(arrays[2].shape, jnp.int32),
            pltpu.VMEM(arrays[3].shape, f32),
            pltpu.VMEM(arrays[5].shape, f32),
            pltpu.VMEM(arrays[6].shape, f32),
            pltpu.VMEM(arrays[4].shape, bf16),
            pltpu.VMEM((cols // 128, channels * rows, 128), f32),
            pltpu.VMEM((channels, cols), f32),
            pltpu.VMEM((3, rows + 2 * REACH, channels, cols), bf16),
            pltpu.VMEM((3, rows + 2 * (REACH - 1), channels, cols), bf16),
            pltpu.VMEM((3, rows + 2 * (REACH - 3), channels, cols), bf16),
            pltpu.VMEM((rows + 2 * (REACH - 1), channels, cols), f32),
            pltpu.VMEM((REACH - LATE, channels, cols), bf16),
            pltpu.VMEM((REACH - LATE, channels, cols), bf16),
            pltpu.VMEM((LAYERS, channels, 9 * channels), bf16),
            pltpu.VMEM((3, 8, cols), f32),
            pltpu.VMEM((8, 128), f32),
            pltpu.VMEM((2, 8, 128), f32),
            pltpu.VMEM((LAYERS, 2, 128), f32),
            pltpu.VMEM((LAYERS, peers, 2, 128), f32),
            pltpu.SemaphoreType.DMA((REACH + 1, 2)),
            pltpu.SemaphoreType.DMA((REACH + 1, 2)),
            pltpu.SemaphoreType.DMA((LAYERS,)),
            pltpu.SemaphoreType.DMA((LAYERS,)),
            pltpu.SemaphoreType.DMA((7,)),
            pltpu.SemaphoreType.REGULAR((max(len(rounds(peers)), 1), 2)),
        ],
        compiler_params=pltpu.CompilerParams(
            collective_id=0, has_side_effects=True, vmem_limit_bytes=44 * 2**20
        ),
    )(*(pltpu.with_memory_space_constraint(array, pltpu.HBM) for array in arrays))
    return pl.pallas_call(
        finish,
        out_shape=jax.ShapeDtypeStruct((channels, rows, cols), bf16),
        in_specs=[vmem] * 3,
        out_specs=pl.BlockSpec(memory_space=pl.ANY),
        scratch_shapes=[
            pltpu.VMEM((cols // 128, channels, rows, 128), bf16),
            pltpu.VMEM((cols // 128, channels * rows, 128), f32),
            pltpu.SemaphoreType.DMA((cols // 128,)),
        ],
        compiler_params=pltpu.CompilerParams(vmem_limit_bytes=8 * 2**20),
    )(own, norm, mask)


def solution(mesh):
    banded = P(None, ("groups", "rows"), None)
    tiled = P(("groups", "rows"), None)
    return jax.shard_map(
        functools.partial(per_device, mesh.shape["rows"]),
        mesh=mesh,
        in_specs=(banded, tiled, tiled, P(), P(), P(), P()),
        out_specs=banded,
        check_vma=False,
    )
```

```python
import functools

import jax
import jax.numpy as jnp
from jax import lax
from jax.experimental import pallas as pl
from jax.experimental.pallas import tpu as pltpu
from jax.sharding import PartitionSpec as P

LAYERS = 3
TILE = 8
STAINS = 4
REACH = 2**LAYERS - 1
EPSILON = 1e-05
NEAR = 4
MID = 2
LATE = 5
MESH = pl.DeviceIdType.MESH
scope = jax.named_scope


def rounds(peers):
    out = []
    reach = NEAR
    while reach < peers - 1:
        out.append(reach)
        reach *= 2
    return tuple(out)


def stack(
    peers,
    slide_ref,
    flags_ref,
    index_ref,
    stain_ref,
    weights_ref,
    gain_ref,
    bias_ref,
    own_ref,
    norm_ref,
    mask_ref,
    slide,
    flags,
    index,
    stain,
    gains,
    biases,
    weights,
    turned,
    scale,
    x0,
    x1,
    x2,
    response,
    mid_out,
    mid_in,
    late_out,
    late_in,
    part,
    near_taps,
    rest_taps,
    taps,
    masks,
    flag_out,
    flag_in,
    tally_out,
    tally_in,
    edge_send,
    edge_recv,
    tally_send,
    tally_recv,
    local_sem,
    far_sem,
):
    channels, rows, cols = slide_ref.shape
    tiles = flags_ref.shape[1]
    bf16, f32 = jnp.bfloat16, jnp.float32
    me = lax.axis_index("rows")
    odd = lax.rem(me, 2)
    turn = 1 - 2 * odd
    partner = (me - turn, me + turn)
    exists = tuple((there >= 0) & (there < peers) for there in partner)
    phase = lax.rem(me, 4)
    through = (phase == 0) | (phase == 3)
    inputs = (x0, x1, x2)
    first = (REACH, REACH - 1, REACH - 3)
    base = REACH - 1
    chunks = cols // 128
    barrier = pltpu.get_barrier_semaphore()

    fetches = {}
    for n, (name, source, target) in enumerate(
        (
            ("flags", flags_ref, flags),
            ("index", index_ref, index),
            ("stain", stain_ref, stain),
            ("slide", slide_ref, slide),
            ("weights", weights_ref, weights),
            ("gain", gain_ref, gains),
            ("bias", bias_ref, biases),
        )
    ):
        fetches[name] = pltpu.make_async_copy(source, target, local_sem.at[n])
        fetches[name].start()

    flag_in[...] = jnp.zeros_like(flag_in)

    def at_distance(distance, side):
        there = me - distance if side == 0 else me + distance
        return there, there >= 0 if side == 0 else there < peers

    for distance in range(1, NEAR + 1):
        for side in range(2):
            there, is_there = at_distance(distance, side)

            @pl.when(is_there)
            def _():
                pl.semaphore_signal(barrier, inc=1, device_id={"rows": there}, device_id_type=MESH)

    far = rounds(peers)

    def far_signal(n):
        for side in range(2):
            there, is_there = at_distance(far[n], side)

            @pl.when(is_there)
            def _():
                pl.semaphore_signal(
                    far_sem.at[n, 1 - side], inc=1, device_id={"rows": there}, device_id_type=MESH
                )

    def far_wait(n):
        for side in range(2):
            _, is_there = at_distance(far[n], side)

            @pl.when(is_there)
            def _():
                pl.semaphore_wait(far_sem.at[n, side], 1)

    spread = (
        lax.broadcasted_iota(jnp.int32, (128, cols), 1) // TILE
        == lax.broadcasted_iota(jnp.int32, (128, cols), 0)
    ).astype(f32)
    eye = lax.broadcasted_iota(jnp.int32, (channels, channels), 0) == lax.broadcasted_iota(
        jnp.int32, (channels, channels), 1
    )

    def column(row):
        return jnp.sum(jnp.where(eye, row, 0.0), axis=1, keepdims=True)

    def as_row(col):
        return jnp.sum(jnp.where(eye, col, 0.0), axis=0, keepdims=True)

    def widen(values):
        return jnp.dot(values, spread, preferred_element_type=f32)

    flag_out[...] = jnp.zeros_like(flag_out)

    with scope("a0_small"):
        fetches["flags"].wait()
        fetches["index"].wait()
        fetches["stain"].wait()
    with scope("a1_scale"):
        flag_out[:, 0:tiles] = jnp.broadcast_to(
            flags[...].astype(f32), (flag_out.shape[0], tiles)
        )
        masks[0] = widen(flag_out[...])
        mask_ref[...] = masks[0]
        classes = jnp.dot(
            jnp.broadcast_to(index[...].astype(f32), (8, tiles)),
            spread[0:tiles],
            preferred_element_type=f32,
        )[0:1]
        factor = jnp.zeros((channels, cols), f32)
        for kind in range(STAINS):
            factor = jnp.where(classes == kind, column(stain[kind : kind + 1, :]), factor)
        scale[...] = factor * masks[0, 0:1, :]
    with scope("a2_slide"):
        fetches["slide"].wait()
    with scope("a3_turn"):
        for at in range(chunks):
            turned[at] = (
                slide[:, :, at * 128 : (at + 1) * 128].astype(f32).reshape(channels * rows, 128)
            )

    lane = lax.broadcasted_iota(jnp.int32, (1, 128), 1)

    def shifts(values, spacing):
        inside = (lane >= spacing).astype(f32).astype(bf16)
        left = pltpu.roll(values, spacing, 1)
        left = jnp.concatenate([left[:, 0:128] * inside, left[:, 128:]], axis=1)
        inside = (lane < 128 - spacing).astype(f32).astype(bf16)
        right = pltpu.roll(values, cols - spacing, 1)
        right = jnp.concatenate([right[:, : cols - 128], right[:, cols - 128 :] * inside], axis=1)
        return left, right

    def place(buffer, row, values, spacing):
        buffer[1, row] = values
        buffer[0, row], buffer[2, row] = shifts(values, spacing)

    def true_row(row):
        return odd * (rows - 1) + turn * row

    def load_row(row):
        values = jnp.concatenate(
            [
                turned[at, pl.ds(true_row(row), channels, stride=rows), :]
                for at in range(chunks)
            ],
            axis=1,
        )
        place(x0, first[0] + row, (values * scale[...]).astype(bf16), 1)

    def edge_copy(piece, side):
        if piece == REACH:
            source, target = flag_out, flag_in.at[side]
        elif side == 0 and piece >= LATE:
            source, target = late_out.at[piece - LATE], late_in.at[piece - LATE]
        elif side == 0 and piece >= MID:
            source, target = mid_out.at[piece - MID], mid_in.at[piece - MID]
        else:
            start = REACH + piece if side == 0 else REACH + rows - 1 - piece
            land = REACH - 1 - piece if side == 0 else REACH + rows + piece
            source, target = x0.at[1, start], x0.at[1, land]
        return pltpu.make_async_remote_copy(
            src_ref=source,
            dst_ref=target,
            send_sem=edge_send.at[piece, side],
            recv_sem=edge_recv.at[piece, side],
            device_id={"rows": partner[side]},
            device_id_type=MESH,
        )

    def send_edges(side, pieces, which=None):
        @pl.when(exists[side] if which is None else exists[side] & which)
        def _():
            for piece in pieces:
                edge_copy(piece, side).start()

    def take_edges(side, pieces):
        @pl.when(exists[side])
        def _():
            for piece in pieces:
                edge_copy(piece, side).wait_recv()

    direct = jnp.logical_not(through)

    with scope("a4_edge_rows"):
        load_row(0)
        load_row(rows - 1)
    with scope("a5_barrier"):
        near = jnp.minimum(me, NEAR) + jnp.minimum(peers - 1 - me, NEAR)
        pl.semaphore_wait(barrier, near)
    with scope("a6_send"):
        send_edges(0, (0,))
        send_edges(1, (0,))
        if far:
            far_signal(0)
    with scope("a7_rows"):
        for row in range(1, rows - 1):
            load_row(row)
        send_edges(0, (1,), direct)
        send_edges(1, range(1, REACH))

        @pl.when(jnp.logical_not(exists[0]))
        def _():
            x0[1, 0:REACH] = jnp.zeros((REACH, channels, cols), bf16)
            mid_in[...] = jnp.zeros_like(mid_in)
            late_in[...] = jnp.zeros_like(late_in)

        @pl.when(jnp.logical_not(exists[1]))
        def _():
            x0[1, REACH + rows : 2 * REACH + rows] = jnp.zeros((REACH, channels, cols), bf16)

    def set_taps(layer):
        for a in range(3):
            for b in range(3):
                tap = 3 * a + b
                taps[layer, :, tap * channels : (tap + 1) * channels] = weights[
                    layer, 3 * (1 + turn * (a - 1)) + b
                ]

    def split_taps():
        for a in range(3):
            for b in range(3):
                target, tap = (near_taps, b) if a == 0 else (rest_taps, 3 * (a - 1) + b)
                target[:, tap * channels : (tap + 1) * channels] = weights[
                    LAYERS - 1, 3 * (1 + turn * (a - 1)) + b
                ]

    with scope("a8_taps"):
        fetches["weights"].wait()
        set_taps(0)

    def place_shifts(row):
        at = first[0] + row
        x0[0, at], x0[2, at] = shifts(x0[1, at], 1)

    def conv_row(layer, row):
        spacing = 2**layer
        source = inputs[layer]
        window = jnp.concatenate(
            [
                source[b, first[layer] + row + (a - 1) * spacing]
                for a in range(3)
                for b in range(3)
            ],
            axis=0,
        )
        return jnp.dot(taps[layer], window, preferred_element_type=f32)

    def halo_row(layer, row):
        response[base + row] = conv_row(layer, row)

    def fold(values):
        total = values[:, 0:128]
        for at in range(128, cols, 128):
            total = total + values[:, at : at + 128]
        return total

    def late_window(row, which):
        step = 2 ** (LAYERS - 1)
        return jnp.concatenate(
            [x2[b, first[2] + row + (a - 1) * step] for a in which for b in range(3)], axis=0
        )

    def own_row(layer, row, carry, late=False):
        sums, squares = carry
        if late:
            own = part[row] + jnp.dot(
                near_taps[...], late_window(row, (0,)), preferred_element_type=f32
            )
        else:
            own = conv_row(layer, row)
        if layer < LAYERS - 1:
            response[base + row] = own
        else:
            for at in range(chunks):
                here = slice(at * 128, (at + 1) * 128)
                own_ref[at, pl.ds(true_row(row), channels, stride=rows), :] = own[:, here]
        masked = own * masks[0, 0:1, :]
        return sums + fold(masked), squares + fold(masked * own)

    def tally(layer, carry):
        sums, squares = carry
        tally_out[layer, 0:1, 0:channels] = as_row(jnp.sum(sums, axis=1, keepdims=True))
        tally_out[layer, 1:2, 0:channels] = as_row(jnp.sum(squares, axis=1, keepdims=True))
        pixels = jnp.sum(masks[0, 0:1, :], axis=1, keepdims=True) * rows
        tally_out[layer, :, channels:] = jnp.broadcast_to(pixels, (2, 128 - channels))
        tally_in[layer, peers - 1] = tally_out[layer]

    def send_tally(layer):
        order = sorted(range(1, peers), key=lambda step: abs(step - peers // 2))
        for step in order:
            pltpu.make_async_remote_copy(
                src_ref=tally_out.at[layer],
                dst_ref=tally_in.at[layer, peers - 1 - step],
                send_sem=tally_send.at[layer],
                recv_sem=tally_recv.at[layer],
                device_id={"rows": lax.rem(me + step, peers)},
                device_id_type=MESH,
            ).start()

    def all_tallies(layer, sem):
        others = tally_in.at[layer, 0 : peers - 1]
        return pltpu.make_async_copy(others, others, sem.at[layer])

    def take_tally(layer):
        all_tallies(layer, tally_recv).wait()
        total = jnp.sum(tally_in[layer], axis=0)
        count = total[0:1, channels : channels + 1]
        average = total[0:1, 0:channels] / count
        variance = jnp.maximum(total[1:2, 0:channels] / count - average * average, 0.0)
        factor = gains[layer : layer + 1, :] * lax.rsqrt(variance + EPSILON)
        return column(average), column(factor), column(biases[layer : layer + 1, :])

    def finish_row(layer, row, norm):
        average, factor, bias = norm
        which = 0 if 0 <= row < rows else 1 if row < 0 else 2
        scaled = ((response[base + row] - average) * factor + bias).astype(bf16)
        mask = masks[which, 0:1, :].astype(bf16)
        values = jnp.maximum(scaled, jnp.zeros((), bf16)) * mask
        place(inputs[layer + 1], first[layer + 1] + row, values, 2 ** (layer + 1))

    def finish_and_conv(layer, order, norm, carry, ready, waiting):
        step = 2 ** (layer + 1)
        for row in order:
            finish_row(layer, row, norm)
            ready.add(row)
            for out in list(waiting):
                if {out - step, out, out + step} <= ready:
                    carry = own_row(layer + 1, out, carry)
                    waiting.remove(out)
        return carry

    nothing = (jnp.zeros((channels, 128), f32),) * 2

    with scope("b0_conv0_inner"):
        carry = nothing
        for row in range(1, rows - 1):
            carry = own_row(0, row, carry)
        centre = jnp.sum(carry[0], axis=1, keepdims=True) / (
            jnp.sum(masks[0, 0:1, :], axis=1, keepdims=True) * (rows - 2)
        )
        for piece in range(MID, LATE):
            mid_out[piece - MID] = (response[base + piece - 1] - centre).astype(bf16)
        flag_out[7:8, 0:channels] = as_row(centre)
        send_edges(0, (REACH,))
        send_edges(1, (REACH,))
        set_taps(1)
        set_taps(2)
        split_taps()
    with scope("b1_far"):
        for n in range(len(far) - 1):
            far_wait(n)
            far_signal(n + 1)
    with scope("b2_fast0"):
        take_edges(1, (0,))
        place_shifts(rows)
        carry = own_row(0, rows - 1, carry)
        send_edges(0, (1,), through)
    with scope("b3_take0"):
        take_edges(0, (0,))
    with scope("b4_slow0"):
        place_shifts(-1)
        carry = own_row(0, 0, carry)
    with scope("b5_far"):
        if far:
            far_wait(len(far) - 1)
    with scope("b6_tally0"):
        tally(0, carry)
        send_tally(0)
        send_edges(0, (2, 3, 4), direct)
        send_edges(0, (2,), through)
    with scope("b7_fast12"):
        fetches["gain"].wait()
        fetches["bias"].wait()
        take_edges(1, (REACH, *range(1, REACH)))
        masks[2] = widen(flag_in[1])
        for piece in range(1, REACH):
            place_shifts(rows + piece)
        for piece in (1, 2):
            halo_row(0, rows - 1 + piece)
    with scope("b8_take1"):
        take_edges(0, (REACH, 1))
    with scope("b8_slow1"):
        masks[1] = widen(flag_in[0])
        place_shifts(-2)
        halo_row(0, -1)
    with scope("b8_fast"):
        for piece in range(3, REACH):
            halo_row(0, rows - 1 + piece)
        send_edges(0, (3,), through)
    with scope("c0_take_tally0"):
        norm0 = take_tally(0)
        near_centre = column(flag_in[0, 7:8, 0:channels])
        send_edges(0, (4,), through)

    def take_mid(piece):
        with scope(f"d{piece}_take"):
            take_edges(0, (piece,))
        response[base - piece] = mid_in[piece - MID].astype(f32) + near_centre

    take_mid(2)
    with scope("c1_layer1"):
        ready, waiting = set(), list(range(rows))
        order = (3, 5, 7, 2, 4, 6, rows, rows + 1, 1, 0, -1, -2)
        carry = finish_and_conv(0, order, norm0, nothing, ready, waiting)
        assert not waiting
    with scope("c2_tally1"):
        tally(1, carry)
        send_tally(1)
    with scope("c3_late"):
        sums = jnp.sum(carry[0], axis=1, keepdims=True)
        pixels = jnp.sum(masks[0, 0:1, :], axis=1, keepdims=True) * rows
        centre = sums / pixels
        for piece in range(LATE, REACH):
            late_out[piece - LATE] = (response[base + piece - 3] - centre).astype(bf16)
            send_edges(0, (piece,), direct)
    with scope("d0_fast"):
        for piece in range(3, REACH):
            finish_row(0, rows - 1 + piece, norm0)
        for piece in range(3, REACH):
            halo_row(1, rows - 3 + piece)

    def slow_piece(piece):
        take_mid(piece)
        with scope(f"d{piece}_work"):
            finish_row(0, -piece, norm0)
            halo_row(1, 2 - piece)

    send_edges(0, (LATE,), through)
    slow_piece(3)
    slow_piece(4)
    send_edges(0, range(LATE + 1, REACH), through)
    with scope("e0_take_tally1"):
        norm1 = take_tally(1)
    ready, waiting = set(), list(range(rows))
    with scope("e1_layer2"):
        order = (11, 7, 3, 10, 6, 9, 5, 8, 4, 2, 1, 0, -1, -2)
        carry = finish_and_conv(1, order, norm1, nothing, ready, waiting)
        for row in waiting:
            part[row] = jnp.dot(
                rest_taps[...], late_window(row, (1, 2)), preferred_element_type=f32
            )
        theirs = tally_in[1, jnp.where(odd == 1, 0, peers - 2)]
        centre = column(theirs[0:1, 0:channels] / theirs[0:1, channels : channels + 1])
    for piece in range(LATE, REACH):
        with scope(f"e{piece}_take"):
            take_edges(0, (piece,))
        with scope(f"e{piece}_late"):
            row = 2 - piece
            response[base + row] = late_in[piece - LATE].astype(f32) + centre
            finish_row(1, row, norm1)
            carry = own_row(2, row + 4, carry, late=True)
            waiting.remove(row + 4)
    assert not waiting
    with scope("e7_tally2"):
        tally(2, carry)
    with scope("e7_send"):
        send_tally(2)
    with scope("e8_sent"):
        for side in range(2):

            @pl.when(exists[side])
            def _():
                for piece in range(REACH + 1):
                    edge_copy(piece, side).wait_send()

        for layer in range(LAYERS):
            all_tallies(layer, tally_send).wait()
    with scope("f0_take_tally2"):
        norm2 = take_tally(2)
    with scope("f1_norm"):
        for n in range(3):
            norm_ref[n] = jnp.broadcast_to(norm2[n], (channels, 128))


def finish(own_ref, norm_ref, mask_ref, out_ref, result, sems):
    channels, rows, cols = out_ref.shape
    part = channels // sems.shape[0]
    masks = [
        jnp.broadcast_to(mask_ref[0:1, at : at + 128], (rows, 128)) for at in range(0, cols, 128)
    ]
    copies = []
    for n in range(sems.shape[0]):
        for channel in range(n * part, (n + 1) * part):
            average, factor, bias = (norm_ref[k, channel : channel + 1, :] for k in range(3))
            for at, mask in enumerate(masks):
                scaled = (own_ref[at, channel * rows : (channel + 1) * rows, :] - average) * factor
                values = jnp.maximum(scaled + bias, 0.0) * mask
                result[channel, :, at * 128 : (at + 1) * 128] = values.astype(result.dtype)
        here = pl.ds(n * part, part)
        copy = pltpu.make_async_copy(result.at[here], out_ref.at[here], sems.at[n])
        copy.start()
        copies.append(copy)
    for copy in copies:
        copy.wait()


def per_device(peers, *arrays):
    channels, rows, cols = arrays[0].shape
    assert rows == TILE and rows > REACH and arrays[1].shape[0] == 1 and channels < 128
    f32, bf16 = jnp.float32, jnp.bfloat16
    vmem = pl.BlockSpec(memory_space=pltpu.VMEM)
    hbm = pl.BlockSpec(memory_space=pltpu.HBM)
    own, norm, mask = pl.pallas_call(
        functools.partial(stack, peers),
        out_shape=(
            jax.ShapeDtypeStruct((cols // 128, channels * rows, 128), f32),
            jax.ShapeDtypeStruct((3, channels, 128), f32),
            jax.ShapeDtypeStruct((8, cols), f32),
        ),
        in_specs=[hbm] * 7,
        out_specs=(vmem,) * 3,
        scratch_shapes=[
            pltpu.VMEM((channels, rows, cols), bf16),
            pltpu.VMEM(arrays[1].shape, jnp.int32),
            pltpu.VMEM(arrays[2].shape, jnp.int32),
            pltpu.VMEM(arrays[3].shape, f32),
            pltpu.VMEM(arrays[5].shape, f32),
            pltpu.VMEM(arrays[6].shape, f32),
            pltpu.VMEM(arrays[4].shape, bf16),
            pltpu.VMEM((cols // 128, channels * rows, 128), f32),
            pltpu.VMEM((channels, cols), f32),
            pltpu.VMEM((3, rows + 2 * REACH, channels, cols), bf16),
            pltpu.VMEM((3, rows + 2 * (REACH - 1), channels, cols), bf16),
            pltpu.VMEM((3, rows + 2 * (REACH - 3), channels, cols), bf16),
            pltpu.VMEM((rows + 2 * (REACH - 1), channels, cols), f32),
            pltpu.VMEM((LATE - MID, channels, cols), bf16),
            pltpu.VMEM((LATE - MID, channels, cols), bf16),
            pltpu.VMEM((REACH - LATE, channels, cols), bf16),
            pltpu.VMEM((REACH - LATE, channels, cols), bf16),
            pltpu.VMEM((REACH - LATE, channels, cols), f32),
            pltpu.VMEM((channels, 3 * channels), bf16),
            pltpu.VMEM((channels, 6 * channels), bf16),
            pltpu.VMEM((LAYERS, channels, 9 * channels), bf16),
            pltpu.VMEM((3, 8, cols), f32),
            pltpu.VMEM((8, 128), f32),
            pltpu.VMEM((2, 8, 128), f32),
            pltpu.VMEM((LAYERS, 2, 128), f32),
            pltpu.VMEM((LAYERS, peers, 2, 128), f32),
            pltpu.SemaphoreType.DMA((REACH + 1, 2)),
            pltpu.SemaphoreType.DMA((REACH + 1, 2)),
            pltpu.SemaphoreType.DMA((LAYERS,)),
            pltpu.SemaphoreType.DMA((LAYERS,)),
            pltpu.SemaphoreType.DMA((7,)),
            pltpu.SemaphoreType.REGULAR((max(len(rounds(peers)), 1), 2)),
        ],
        compiler_params=pltpu.CompilerParams(
            collective_id=0, has_side_effects=True, vmem_limit_bytes=44 * 2**20
        ),
    )(*(pltpu.with_memory_space_constraint(array, pltpu.HBM) for array in arrays))
    return pl.pallas_call(
        finish,
        out_shape=jax.ShapeDtypeStruct((channels, rows, cols), bf16),
        in_specs=[vmem] * 3,
        out_specs=pl.BlockSpec(memory_space=pl.ANY),
        scratch_shapes=[
            pltpu.VMEM((channels, rows, cols), bf16),
            pltpu.SemaphoreType.DMA((4 if channels % 4 == 0 else 1,)),
        ],
        compiler_params=pltpu.CompilerParams(vmem_limit_bytes=8 * 2**20),
    )(own, norm, mask)


def solution(mesh):
    banded = P(None, ("groups", "rows"), None)
    tiled = P(("groups", "rows"), None)
    return jax.shard_map(
        functools.partial(per_device, mesh.shape["rows"]),
        mesh=mesh,
        in_specs=(banded, tiled, tiled, P(), P(), P(), P()),
        out_specs=banded,
        check_vma=False,
    )
```

```python
import functools

import jax
import jax.numpy as jnp
from jax import lax
from jax.experimental import pallas as pl
from jax.experimental.pallas import tpu as pltpu
from jax.sharding import PartitionSpec as P

LAYERS = 3
TILE = 8
STAINS = 4
REACH = 2**LAYERS - 1
EPSILON = 1e-05
NEAR = 4
MID = 2
LATE = 5
MESH = pl.DeviceIdType.MESH
scope = jax.named_scope


def rounds(peers):
    out = []
    reach = NEAR
    while reach < peers - 1:
        out.append(reach)
        reach *= 2
    return tuple(out)


def stack(
    peers,
    slide_ref,
    flags_ref,
    index_ref,
    stain_ref,
    weights_ref,
    gain_ref,
    bias_ref,
    own_ref,
    norm_ref,
    mask_ref,
    slide,
    flags,
    index,
    stain,
    gains,
    biases,
    weights,
    turned,
    scale,
    x0,
    x1,
    x2,
    response,
    mid_out,
    mid_in,
    late_out,
    late_in,
    part,
    near_taps,
    rest_taps,
    taps,
    masks,
    flag_out,
    flag_in,
    tally_out,
    tally_in,
    edge_send,
    edge_recv,
    tally_send,
    tally_recv,
    local_sem,
    far_sem,
):
    channels, rows, cols = slide_ref.shape
    tiles = flags_ref.shape[1]
    bf16, f32 = jnp.bfloat16, jnp.float32
    me = lax.axis_index("rows")
    odd = lax.rem(me, 2)
    turn = 1 - 2 * odd
    partner = (me - turn, me + turn)
    exists = tuple((there >= 0) & (there < peers) for there in partner)
    phase = lax.rem(me, 4)
    through = (phase == 0) | (phase == 3)
    inputs = (x0, x1, x2)
    first = (REACH, REACH - 1, REACH - 3)
    base = REACH - 1
    chunks = cols // 128
    barrier = pltpu.get_barrier_semaphore()

    fetches = {}
    for n, (name, source, target) in enumerate(
        (
            ("flags", flags_ref, flags),
            ("index", index_ref, index),
            ("stain", stain_ref, stain),
            ("slide", slide_ref, slide),
            ("weights", weights_ref, weights),
            ("gain", gain_ref, gains),
            ("bias", bias_ref, biases),
        )
    ):
        fetches[name] = pltpu.make_async_copy(source, target, local_sem.at[n % 5])
        if n < 5:
            fetches[name].start()

    flag_in[...] = jnp.zeros_like(flag_in)

    def at_distance(distance, side):
        there = me - distance if side == 0 else me + distance
        return there, there >= 0 if side == 0 else there < peers

    for distance in range(1, NEAR + 1):
        for side in range(2):
            there, is_there = at_distance(distance, side)

            @pl.when(is_there)
            def _():
                pl.semaphore_signal(barrier, inc=1, device_id={"rows": there}, device_id_type=MESH)

    far = rounds(peers)

    def far_signal(n):
        for side in range(2):
            there, is_there = at_distance(far[n], side)

            @pl.when(is_there)
            def _():
                pl.semaphore_signal(
                    far_sem.at[n], inc=1, device_id={"rows": there}, device_id_type=MESH
                )

    def far_wait(n):
        there = jnp.where(me >= far[n], 1, 0) + jnp.where(me + far[n] < peers, 1, 0)

        @pl.when(there > 0)
        def _():
            pl.semaphore_wait(far_sem.at[n], there)

    spread = (
        lax.broadcasted_iota(jnp.int32, (128, cols), 1) // TILE
        == lax.broadcasted_iota(jnp.int32, (128, cols), 0)
    ).astype(f32)
    eye = lax.broadcasted_iota(jnp.int32, (channels, channels), 0) == lax.broadcasted_iota(
        jnp.int32, (channels, channels), 1
    )

    def column(row):
        return jnp.sum(jnp.where(eye, row, 0.0), axis=1, keepdims=True)

    def as_row(col):
        return jnp.sum(jnp.where(eye, col, 0.0), axis=0, keepdims=True)

    def widen(values):
        return jnp.dot(values, spread, preferred_element_type=f32)

    flag_out[...] = jnp.zeros_like(flag_out)

    with scope("a0_small"):
        fetches["flags"].wait()
        fetches["index"].wait()
        fetches["stain"].wait()
        fetches["gain"].start()
        fetches["bias"].start()
    with scope("a1_scale"):
        flag_out[:, 0:tiles] = jnp.broadcast_to(
            flags[...].astype(f32), (flag_out.shape[0], tiles)
        )
        masks[0] = widen(flag_out[...])
        mask_ref[...] = masks[0]
        classes = jnp.dot(
            jnp.broadcast_to(index[...].astype(f32), (8, tiles)),
            spread[0:tiles],
            preferred_element_type=f32,
        )[0:1]
        factor = jnp.zeros((channels, cols), f32)
        for kind in range(STAINS):
            factor = jnp.where(classes == kind, column(stain[kind : kind + 1, :]), factor)
        scale[...] = factor * masks[0, 0:1, :]
    with scope("a2_slide"):
        fetches["slide"].wait()
    with scope("a3_turn"):
        for at in range(chunks):
            turned[at] = (
                slide[:, :, at * 128 : (at + 1) * 128].astype(f32).reshape(channels * rows, 128)
            )

    lane = lax.broadcasted_iota(jnp.int32, (1, 128), 1)

    def shifts(values, spacing):
        inside = (lane >= spacing).astype(f32).astype(bf16)
        left = pltpu.roll(values, spacing, 1)
        left = jnp.concatenate([left[:, 0:128] * inside, left[:, 128:]], axis=1)
        inside = (lane < 128 - spacing).astype(f32).astype(bf16)
        right = pltpu.roll(values, cols - spacing, 1)
        right = jnp.concatenate([right[:, : cols - 128], right[:, cols - 128 :] * inside], axis=1)
        return left, right

    def place(buffer, row, values, spacing):
        buffer[1, row] = values
        buffer[0, row], buffer[2, row] = shifts(values, spacing)

    def true_row(row):
        return odd * (rows - 1) + turn * row

    def load_row(row):
        values = jnp.concatenate(
            [
                turned[at, pl.ds(true_row(row), channels, stride=rows), :]
                for at in range(chunks)
            ],
            axis=1,
        )
        place(x0, first[0] + row, (values * scale[...]).astype(bf16), 1)

    def arrival(piece, side):
        if piece == REACH:
            return 0
        if side == 1:
            return 1 if piece == 0 else 2
        return 1 if piece == LATE + 1 else 3 + piece % LATE

    def edge_copy(piece, side):
        if piece == REACH:
            source, target = flag_out, flag_in.at[side]
        elif side == 0 and piece >= LATE:
            source, target = late_out.at[piece - LATE], late_in.at[piece - LATE]
        elif side == 0 and piece >= MID:
            source, target = mid_out.at[piece - MID], mid_in.at[piece - MID]
        else:
            start = REACH + piece if side == 0 else REACH + rows - 1 - piece
            land = REACH - 1 - piece if side == 0 else REACH + rows + piece
            source, target = x0.at[1, start], x0.at[1, land]
        return pltpu.make_async_remote_copy(
            src_ref=source,
            dst_ref=target,
            send_sem=edge_send.at[2 if piece == REACH else side],
            recv_sem=edge_recv.at[arrival(piece, side)],
            device_id={"rows": partner[side]},
            device_id_type=MESH,
        )

    def send_edges(side, pieces, which=None):
        @pl.when(exists[side] if which is None else exists[side] & which)
        def _():
            for piece in pieces:
                edge_copy(piece, side).start()

    def take_edges(side, pieces):
        @pl.when(exists[side])
        def _():
            for piece in pieces:
                edge_copy(piece, side).wait_recv()

    def if_there(side, act):
        @pl.when(exists[side])
        def _():
            act()

    def flags_done(sem):
        both = exists[0] & exists[1]

        @pl.when(both)
        def _():
            pltpu.make_async_copy(flag_in, flag_in, sem).wait()

        @pl.when((exists[0] | exists[1]) & jnp.logical_not(both))
        def _():
            pltpu.make_async_copy(flag_out, flag_out, sem).wait()

    direct = jnp.logical_not(through)

    with scope("a4_edge_rows"):
        load_row(0)
        load_row(rows - 1)
    with scope("a5_barrier"):
        near = jnp.minimum(me, NEAR) + jnp.minimum(peers - 1 - me, NEAR)
        pl.semaphore_wait(barrier, near)
    with scope("a6_send"):
        send_edges(0, (0,))
        send_edges(1, (0,))
        if far:
            far_signal(0)
    with scope("a7_rows"):
        for row in range(1, rows - 1):
            load_row(row)
        send_edges(0, (1,), direct)
        send_edges(1, range(1, REACH))

        @pl.when(jnp.logical_not(exists[0]))
        def _():
            x0[1, 0:REACH] = jnp.zeros((REACH, channels, cols), bf16)
            mid_in[...] = jnp.zeros_like(mid_in)
            late_in[...] = jnp.zeros_like(late_in)

        @pl.when(jnp.logical_not(exists[1]))
        def _():
            x0[1, REACH + rows : 2 * REACH + rows] = jnp.zeros((REACH, channels, cols), bf16)

    def set_taps(layer):
        for a in range(3):
            for b in range(3):
                tap = 3 * a + b
                taps[layer, :, tap * channels : (tap + 1) * channels] = weights[
                    layer, 3 * (1 + turn * (a - 1)) + b
                ]

    def split_taps():
        for a in range(3):
            for b in range(3):
                target, tap = (near_taps, b) if a == 0 else (rest_taps, 3 * (a - 1) + b)
                target[:, tap * channels : (tap + 1) * channels] = weights[
                    LAYERS - 1, 3 * (1 + turn * (a - 1)) + b
                ]

    with scope("a8_taps"):
        fetches["weights"].wait()
        set_taps(0)

    def place_shifts(row):
        at = first[0] + row
        x0[0, at], x0[2, at] = shifts(x0[1, at], 1)

    def conv_row(layer, row):
        spacing = 2**layer
        source = inputs[layer]
        window = jnp.concatenate(
            [
                source[b, first[layer] + row + (a - 1) * spacing]
                for a in range(3)
                for b in range(3)
            ],
            axis=0,
        )
        return jnp.dot(taps[layer], window, preferred_element_type=f32)

    def halo_row(layer, row):
        response[base + row] = conv_row(layer, row)

    def fold(values):
        total = values[:, 0:128]
        for at in range(128, cols, 128):
            total = total + values[:, at : at + 128]
        return total

    def late_window(row, which):
        step = 2 ** (LAYERS - 1)
        return jnp.concatenate(
            [x2[b, first[2] + row + (a - 1) * step] for a in which for b in range(3)], axis=0
        )

    def own_row(layer, row, carry, late=False):
        sums, squares = carry
        if late:
            own = part[row] + jnp.dot(
                near_taps[...], late_window(row, (0,)), preferred_element_type=f32
            )
        else:
            own = conv_row(layer, row)
        if layer < LAYERS - 1:
            response[base + row] = own
        else:
            for at in range(chunks):
                here = slice(at * 128, (at + 1) * 128)
                own_ref[at, pl.ds(true_row(row), channels, stride=rows), :] = own[:, here]
        masked = own * masks[0, 0:1, :]
        return sums + fold(masked), squares + fold(masked * own)

    def tally(layer, carry):
        sums, squares = carry
        tally_out[layer, 0:1, 0:channels] = as_row(jnp.sum(sums, axis=1, keepdims=True))
        tally_out[layer, 1:2, 0:channels] = as_row(jnp.sum(squares, axis=1, keepdims=True))
        pixels = jnp.sum(masks[0, 0:1, :], axis=1, keepdims=True) * rows
        tally_out[layer, :, channels:] = jnp.broadcast_to(pixels, (2, 128 - channels))
        tally_in[layer, peers - 1] = tally_out[layer]

    def send_tally(layer):
        order = sorted(range(1, peers), key=lambda step: abs(step - peers // 2))
        for step in order:
            pltpu.make_async_remote_copy(
                src_ref=tally_out.at[layer],
                dst_ref=tally_in.at[layer, peers - 1 - step],
                send_sem=tally_send.at[0],
                recv_sem=tally_recv.at[layer % 2],
                device_id={"rows": lax.rem(me + step, peers)},
                device_id_type=MESH,
            ).start()

    def all_tallies(layer, sem):
        others = tally_in.at[layer, 0 : peers - 1]
        return pltpu.make_async_copy(others, others, sem)

    def take_tally(layer):
        all_tallies(layer, tally_recv.at[layer % 2]).wait()
        total = jnp.sum(tally_in[layer], axis=0)
        count = total[0:1, channels : channels + 1]
        average = total[0:1, 0:channels] / count
        variance = jnp.maximum(total[1:2, 0:channels] / count - average * average, 0.0)
        factor = gains[layer : layer + 1, :] * lax.rsqrt(variance + EPSILON)
        return column(average), column(factor), column(biases[layer : layer + 1, :])

    def finish_row(layer, row, norm):
        average, factor, bias = norm
        which = 0 if 0 <= row < rows else 1 if row < 0 else 2
        scaled = ((response[base + row] - average) * factor + bias).astype(bf16)
        mask = masks[which, 0:1, :].astype(bf16)
        values = jnp.maximum(scaled, jnp.zeros((), bf16)) * mask
        place(inputs[layer + 1], first[layer + 1] + row, values, 2 ** (layer + 1))

    def finish_and_conv(layer, order, norm, carry, ready, waiting):
        step = 2 ** (layer + 1)
        for row in order:
            finish_row(layer, row, norm)
            ready.add(row)
            for out in list(waiting):
                if {out - step, out, out + step} <= ready:
                    carry = own_row(layer + 1, out, carry)
                    waiting.remove(out)
        return carry

    nothing = (jnp.zeros((channels, 128), f32),) * 2

    with scope("b0_conv0_inner"):
        carry = nothing
        for row in range(1, rows - 1):
            carry = own_row(0, row, carry)
        centre = jnp.sum(carry[0], axis=1, keepdims=True) / (
            jnp.sum(masks[0, 0:1, :], axis=1, keepdims=True) * (rows - 2)
        )
        for piece in range(MID, LATE):
            mid_out[piece - MID] = (response[base + piece - 1] - centre).astype(bf16)
        flag_out[7:8, 0:channels] = as_row(centre)
        send_edges(0, (REACH,))
        send_edges(1, (REACH,))
        send_edges(0, (2,), phase == 1)
        set_taps(1)
        set_taps(2)
        split_taps()
    with scope("b1_far"):
        for n in range(len(far) - 1):
            far_wait(n)
            far_signal(n + 1)
    with scope("b2_fast0"):
        take_edges(1, (0,))
        place_shifts(rows)
        carry = own_row(0, rows - 1, carry)
        send_edges(0, (1,), through)
    with scope("b3_take0"):
        take_edges(0, (0,))
    with scope("b4_slow0"):
        place_shifts(-1)
        carry = own_row(0, 0, carry)
    with scope("b5_far"):
        if far:
            far_wait(len(far) - 1)
    with scope("b6_tally0"):
        tally(0, carry)
        send_tally(0)
        send_edges(0, (3, 4), phase == 1)
        send_edges(0, (2, 3, 4), phase == 2)
        send_edges(0, (2,), through)
    with scope("b7_fast12"):
        fetches["gain"].wait()
        fetches["bias"].wait()
        rest = x0.at[1, REACH + rows + 1 : 2 * REACH + rows]
        if_there(1, lambda: pltpu.make_async_copy(rest, rest, edge_recv.at[2]).wait())
        for piece in range(1, REACH):
            place_shifts(rows + piece)
        for piece in (1, 2):
            halo_row(0, rows - 1 + piece)
    with scope("b8_take1"):
        take_edges(0, (1,))
        flags_done(edge_recv.at[0])
    with scope("b8_slow1"):
        masks[1] = widen(flag_in[0])
        masks[2] = widen(flag_in[1])
        place_shifts(-2)
        halo_row(0, -1)
    with scope("b8_fast"):
        for piece in range(3, REACH):
            halo_row(0, rows - 1 + piece)
        send_edges(0, (3,), through)
    with scope("c0_take_tally0"):
        norm0 = take_tally(0)
        all_tallies(0, tally_send.at[0]).wait()
        near_centre = column(flag_in[0, 7:8, 0:channels])
        send_edges(0, (4,), through)

    def take_mid(piece):
        with scope(f"d{piece}_take"):
            take_edges(0, (piece,))
        response[base - piece] = mid_in[piece - MID].astype(f32) + near_centre

    take_mid(2)
    with scope("c1_layer1"):
        ready, waiting = set(), list(range(rows))
        order = (3, 5, 7, 2, 4, 6, rows, rows + 1, 1, 0, -1, -2)
        carry = finish_and_conv(0, order, norm0, nothing, ready, waiting)
        assert not waiting
    with scope("c2_tally1"):
        tally(1, carry)
        send_tally(1)
    with scope("c3_late"):
        sums = jnp.sum(carry[0], axis=1, keepdims=True)
        pixels = jnp.sum(masks[0, 0:1, :], axis=1, keepdims=True) * rows
        centre = sums / pixels
        for piece in range(LATE, REACH):
            late_out[piece - LATE] = (response[base + piece - 3] - centre).astype(bf16)
            send_edges(0, (piece,), direct)
    with scope("d0_fast"):
        for piece in range(3, REACH):
            finish_row(0, rows - 1 + piece, norm0)
        for piece in range(3, REACH):
            halo_row(1, rows - 3 + piece)

    def slow_piece(piece):
        take_mid(piece)
        with scope(f"d{piece}_work"):
            finish_row(0, -piece, norm0)
            halo_row(1, 2 - piece)

    send_edges(0, (LATE,), through)
    slow_piece(3)
    slow_piece(4)
    send_edges(0, range(LATE + 1, REACH), through)
    with scope("e0_take_tally1"):
        norm1 = take_tally(1)
        all_tallies(1, tally_send.at[0]).wait()
    ready, waiting = set(), list(range(rows))
    with scope("e1_layer2"):
        order = (11, 7, 3, 10, 6, 9, 5, 8, 4, 2, 1, 0, -1, -2)
        carry = finish_and_conv(1, order, norm1, nothing, ready, waiting)
        for row in waiting:
            part[row] = jnp.dot(
                rest_taps[...], late_window(row, (1, 2)), preferred_element_type=f32
            )
        theirs = tally_in[1, jnp.where(odd == 1, 0, peers - 2)]
        centre = column(theirs[0:1, 0:channels] / theirs[0:1, channels : channels + 1])
    for piece in range(LATE, REACH):
        with scope(f"e{piece}_take"):
            take_edges(0, (piece,))
        with scope(f"e{piece}_late"):
            row = 2 - piece
            response[base + row] = late_in[piece - LATE].astype(f32) + centre
            finish_row(1, row, norm1)
            carry = own_row(2, row + 4, carry, late=True)
            waiting.remove(row + 4)
    assert not waiting
    with scope("e7_tally2"):
        tally(2, carry)
    with scope("e7_send"):
        send_tally(2)
    with scope("e8_sent"):
        sent = x0.at[1, 0:REACH]
        for side in range(2):
            if_there(side, lambda: pltpu.make_async_copy(sent, sent, edge_send.at[side]).wait())
        flags_done(edge_send.at[2])
        all_tallies(2, tally_send.at[0]).wait()
    with scope("f0_take_tally2"):
        norm2 = take_tally(2)
    with scope("f1_norm"):
        for n in range(3):
            norm_ref[n] = jnp.broadcast_to(norm2[n], (channels, 128))


def finish(own_ref, norm_ref, mask_ref, out_ref, result, sems):
    channels, rows, cols = out_ref.shape
    part = channels // sems.shape[0]
    masks = [
        jnp.broadcast_to(mask_ref[0:1, at : at + 128], (rows, 128)) for at in range(0, cols, 128)
    ]
    copies = []
    for n in range(sems.shape[0]):
        for channel in range(n * part, (n + 1) * part):
            average, factor, bias = (norm_ref[k, channel : channel + 1, :] for k in range(3))
            for at, mask in enumerate(masks):
                scaled = (own_ref[at, channel * rows : (channel + 1) * rows, :] - average) * factor
                values = jnp.maximum(scaled + bias, 0.0) * mask
                result[channel, :, at * 128 : (at + 1) * 128] = values.astype(result.dtype)
        here = pl.ds(n * part, part)
        copy = pltpu.make_async_copy(result.at[here], out_ref.at[here], sems.at[n])
        copy.start()
        copies.append(copy)
    for copy in copies:
        copy.wait()


def per_device(peers, *arrays):
    channels, rows, cols = arrays[0].shape
    assert rows == TILE and rows > REACH and arrays[1].shape[0] == 1 and channels < 128
    f32, bf16 = jnp.float32, jnp.bfloat16
    vmem = pl.BlockSpec(memory_space=pltpu.VMEM)
    hbm = pl.BlockSpec(memory_space=pltpu.HBM)
    own, norm, mask = pl.pallas_call(
        functools.partial(stack, peers),
        out_shape=(
            jax.ShapeDtypeStruct((cols // 128, channels * rows, 128), f32),
            jax.ShapeDtypeStruct((3, channels, 128), f32),
            jax.ShapeDtypeStruct((8, cols), f32),
        ),
        in_specs=[hbm] * 7,
        out_specs=(vmem,) * 3,
        scratch_shapes=[
            pltpu.VMEM((channels, rows, cols), bf16),
            pltpu.VMEM(arrays[1].shape, jnp.int32),
            pltpu.VMEM(arrays[2].shape, jnp.int32),
            pltpu.VMEM(arrays[3].shape, f32),
            pltpu.VMEM(arrays[5].shape, f32),
            pltpu.VMEM(arrays[6].shape, f32),
            pltpu.VMEM(arrays[4].shape, bf16),
            pltpu.VMEM((cols // 128, channels * rows, 128), f32),
            pltpu.VMEM((channels, cols), f32),
            pltpu.VMEM((3, rows + 2 * REACH, channels, cols), bf16),
            pltpu.VMEM((3, rows + 2 * (REACH - 1), channels, cols), bf16),
            pltpu.VMEM((3, rows + 2 * (REACH - 3), channels, cols), bf16),
            pltpu.VMEM((rows + 2 * (REACH - 1), channels, cols), f32),
            pltpu.VMEM((LATE - MID, channels, cols), bf16),
            pltpu.VMEM((LATE - MID, channels, cols), bf16),
            pltpu.VMEM((REACH - LATE, channels, cols), bf16),
            pltpu.VMEM((REACH - LATE, channels, cols), bf16),
            pltpu.VMEM((REACH - LATE, channels, cols), f32),
            pltpu.VMEM((channels, 3 * channels), bf16),
            pltpu.VMEM((channels, 6 * channels), bf16),
            pltpu.VMEM((LAYERS, channels, 9 * channels), bf16),
            pltpu.VMEM((3, 8, cols), f32),
            pltpu.VMEM((8, 128), f32),
            pltpu.VMEM((2, 8, 128), f32),
            pltpu.VMEM((LAYERS, 2, 128), f32),
            pltpu.VMEM((LAYERS, peers, 2, 128), f32),
            pltpu.SemaphoreType.DMA((3,)),
            pltpu.SemaphoreType.DMA((3 + LATE,)),
            pltpu.SemaphoreType.DMA((1,)),
            pltpu.SemaphoreType.DMA((2,)),
            pltpu.SemaphoreType.DMA((5,)),
            pltpu.SemaphoreType.REGULAR((max(len(rounds(peers)), 1),)),
        ],
        compiler_params=pltpu.CompilerParams(
            collective_id=0, has_side_effects=True, vmem_limit_bytes=44 * 2**20
        ),
    )(*(pltpu.with_memory_space_constraint(array, pltpu.HBM) for array in arrays))
    return pl.pallas_call(
        finish,
        out_shape=jax.ShapeDtypeStruct((channels, rows, cols), bf16),
        in_specs=[vmem] * 3,
        out_specs=pl.BlockSpec(memory_space=pl.ANY),
        scratch_shapes=[
            pltpu.VMEM((channels, rows, cols), bf16),
            pltpu.SemaphoreType.DMA((4 if channels % 4 == 0 else 1,)),
        ],
        compiler_params=pltpu.CompilerParams(vmem_limit_bytes=8 * 2**20),
    )(own, norm, mask)


def solution(mesh):
    banded = P(None, ("groups", "rows"), None)
    tiled = P(("groups", "rows"), None)
    return jax.shard_map(
        functools.partial(per_device, mesh.shape["rows"]),
        mesh=mesh,
        in_specs=(banded, tiled, tiled, P(), P(), P(), P()),
        out_specs=banded,
        check_vma=False,
    )
```

```python
import functools

import jax
import jax.numpy as jnp
from jax import lax
from jax.experimental import pallas as pl
from jax.experimental.pallas import tpu as pltpu
from jax.sharding import PartitionSpec as P

LAYERS = 3
TILE = 8
STAINS = 4
REACH = 2**LAYERS - 1
EPSILON = 1e-05
NEAR = 4
MID = 2
LATE = 5
MESH = pl.DeviceIdType.MESH
scope = jax.named_scope


def rounds(peers):
    out = []
    reach = NEAR
    while reach < peers - 1:
        out.append(reach)
        reach *= 2
    return tuple(out)


def stack(
    peers,
    slide_ref,
    flags_ref,
    index_ref,
    stain_ref,
    weights_ref,
    gain_ref,
    bias_ref,
    own_ref,
    norm_ref,
    mask_ref,
    slide,
    flags,
    index,
    stain,
    gains,
    biases,
    weights,
    turned,
    scale,
    x0,
    x1,
    x2,
    response,
    mid_out,
    mid_in,
    late_out,
    late_in,
    part,
    near_taps,
    rest_taps,
    taps,
    masks,
    flag_out,
    flag_in,
    tally_out,
    tally_in,
    edge_send,
    edge_recv,
    tally_send,
    tally_recv,
    local_sem,
    far_sem,
):
    channels, rows, cols = slide_ref.shape
    tiles = flags_ref.shape[1]
    bf16, f32 = jnp.bfloat16, jnp.float32
    me = lax.axis_index("rows")
    odd = lax.rem(me, 2)
    turn = 1 - 2 * odd
    partner = (me - turn, me + turn)
    exists = tuple((there >= 0) & (there < peers) for there in partner)
    phase = lax.rem(me, 4)
    through = (phase == 0) | (phase == 3)
    inputs = (x0, x1, x2)
    first = (REACH, REACH - 1, REACH - 3)
    base = REACH - 1
    chunks = cols // 128
    barrier = pltpu.get_barrier_semaphore()

    fetches = {}
    for n, (name, source, target) in enumerate(
        (
            ("flags", flags_ref, flags),
            ("index", index_ref, index),
            ("stain", stain_ref, stain),
            ("slide", slide_ref, slide),
            ("weights", weights_ref, weights),
            ("gain", gain_ref, gains),
            ("bias", bias_ref, biases),
        )
    ):
        fetches[name] = pltpu.make_async_copy(source, target, local_sem.at[n % 5])
        if n < 5:
            fetches[name].start()

    flag_in[...] = jnp.zeros_like(flag_in)

    def at_distance(distance, side):
        there = me - distance if side == 0 else me + distance
        return there, there >= 0 if side == 0 else there < peers

    for distance in range(1, NEAR + 1):
        for side in range(2):
            there, is_there = at_distance(distance, side)

            @pl.when(is_there)
            def _():
                pl.semaphore_signal(barrier, inc=1, device_id={"rows": there}, device_id_type=MESH)

    far = rounds(peers)

    def far_signal(n):
        for side in range(2):
            there, is_there = at_distance(far[n], side)

            @pl.when(is_there)
            def _():
                pl.semaphore_signal(
                    far_sem.at[n], inc=1, device_id={"rows": there}, device_id_type=MESH
                )

    def far_wait(n):
        there = jnp.where(me >= far[n], 1, 0) + jnp.where(me + far[n] < peers, 1, 0)

        @pl.when(there > 0)
        def _():
            pl.semaphore_wait(far_sem.at[n], there)

    spread = (
        lax.broadcasted_iota(jnp.int32, (128, cols), 1) // TILE
        == lax.broadcasted_iota(jnp.int32, (128, cols), 0)
    ).astype(f32)
    eye = lax.broadcasted_iota(jnp.int32, (channels, channels), 0) == lax.broadcasted_iota(
        jnp.int32, (channels, channels), 1
    )

    def column(row):
        return jnp.sum(jnp.where(eye, row, 0.0), axis=1, keepdims=True)

    def as_row(col):
        return jnp.sum(jnp.where(eye, col, 0.0), axis=0, keepdims=True)

    def widen(values):
        return jnp.dot(values, spread, preferred_element_type=f32)

    flag_out[...] = jnp.zeros_like(flag_out)

    with scope("a0_small"):
        fetches["flags"].wait()
        fetches["index"].wait()
        fetches["stain"].wait()
        fetches["gain"].start()
        fetches["bias"].start()
    with scope("a1_scale"):
        flag_out[:, 0:tiles] = jnp.broadcast_to(
            flags[...].astype(f32), (flag_out.shape[0], tiles)
        )
        masks[0] = widen(flag_out[...])
        mask_ref[...] = masks[0]
        classes = jnp.dot(
            jnp.broadcast_to(index[...].astype(f32), (8, tiles)),
            spread[0:tiles],
            preferred_element_type=f32,
        )[0:1]
        factor = jnp.zeros((channels, cols), f32)
        for kind in range(STAINS):
            factor = jnp.where(classes == kind, column(stain[kind : kind + 1, :]), factor)
        scale[...] = factor * masks[0, 0:1, :]
    with scope("a2_slide"):
        fetches["slide"].wait()
    with scope("a3_turn"):
        for at in range(chunks):
            turned[at] = (
                slide[:, :, at * 128 : (at + 1) * 128].astype(f32).reshape(channels * rows, 128)
            )

    lane = lax.broadcasted_iota(jnp.int32, (1, 128), 1)

    def shifts(values, spacing):
        inside = (lane >= spacing).astype(f32).astype(bf16)
        left = pltpu.roll(values, spacing, 1)
        left = jnp.concatenate([left[:, 0:128] * inside, left[:, 128:]], axis=1)
        inside = (lane < 128 - spacing).astype(f32).astype(bf16)
        right = pltpu.roll(values, cols - spacing, 1)
        right = jnp.concatenate([right[:, : cols - 128], right[:, cols - 128 :] * inside], axis=1)
        return left, right

    def place(buffer, row, values, spacing):
        buffer[1, row] = values
        buffer[0, row], buffer[2, row] = shifts(values, spacing)

    def true_row(row):
        return odd * (rows - 1) + turn * row

    def load_row(row):
        values = jnp.concatenate(
            [
                turned[at, pl.ds(true_row(row), channels, stride=rows), :]
                for at in range(chunks)
            ],
            axis=1,
        )
        place(x0, first[0] + row, (values * scale[...]).astype(bf16), 1)

    def arrival(piece, side):
        if piece == REACH:
            return 0
        if side == 1:
            return 1 if piece == 0 else 2
        return 1 if piece == LATE + 1 else 3 + piece % LATE

    def edge_copy(piece, side):
        if piece == REACH:
            source, target = flag_out, flag_in.at[side]
        elif side == 0 and piece >= LATE:
            source, target = late_out.at[piece - LATE], late_in.at[piece - LATE]
        elif side == 0 and piece >= MID:
            source, target = mid_out.at[piece - MID], mid_in.at[piece - MID]
        else:
            start = REACH + piece if side == 0 else REACH + rows - 1 - piece
            land = REACH - 1 - piece if side == 0 else REACH + rows + piece
            source, target = x0.at[1, start], x0.at[1, land]
        return pltpu.make_async_remote_copy(
            src_ref=source,
            dst_ref=target,
            send_sem=edge_send.at[2 if piece == REACH else side],
            recv_sem=edge_recv.at[arrival(piece, side)],
            device_id={"rows": partner[side]},
            device_id_type=MESH,
        )

    def send_edges(side, pieces, which=None):
        @pl.when(exists[side] if which is None else exists[side] & which)
        def _():
            for piece in pieces:
                edge_copy(piece, side).start()

    def take_edges(side, pieces):
        @pl.when(exists[side])
        def _():
            for piece in pieces:
                edge_copy(piece, side).wait_recv()

    def if_there(side, act):
        @pl.when(exists[side])
        def _():
            act()

    def flags_done(sem):
        both = exists[0] & exists[1]

        @pl.when(both)
        def _():
            pltpu.make_async_copy(flag_in, flag_in, sem).wait()

        @pl.when((exists[0] | exists[1]) & jnp.logical_not(both))
        def _():
            pltpu.make_async_copy(flag_out, flag_out, sem).wait()

    direct = jnp.logical_not(through)

    with scope("a4_edge_rows"):
        load_row(0)
        load_row(rows - 1)
    with scope("a5_barrier"):
        near = jnp.minimum(me, NEAR) + jnp.minimum(peers - 1 - me, NEAR)
        pl.semaphore_wait(barrier, near)
    with scope("a6_send"):
        send_edges(0, (0,))
        send_edges(1, (0,))
        if far:
            far_signal(0)
    with scope("a7_rows"):
        for row in range(1, rows - 1):
            load_row(row)
        send_edges(0, (1,), direct)
        send_edges(1, range(1, REACH))

        @pl.when(jnp.logical_not(exists[0]))
        def _():
            x0[1, 0:REACH] = jnp.zeros((REACH, channels, cols), bf16)
            mid_in[...] = jnp.zeros_like(mid_in)
            late_in[...] = jnp.zeros_like(late_in)

        @pl.when(jnp.logical_not(exists[1]))
        def _():
            x0[1, REACH + rows : 2 * REACH + rows] = jnp.zeros((REACH, channels, cols), bf16)

    def set_taps(layer):
        for a in range(3):
            for b in range(3):
                tap = 3 * a + b
                taps[layer, :, tap * channels : (tap + 1) * channels] = weights[
                    layer, 3 * (1 + turn * (a - 1)) + b
                ]

    def split_taps():
        for a in range(3):
            for b in range(3):
                target, tap = (near_taps, b) if a == 0 else (rest_taps, 3 * (a - 1) + b)
                target[:, tap * channels : (tap + 1) * channels] = weights[
                    LAYERS - 1, 3 * (1 + turn * (a - 1)) + b
                ]

    with scope("a8_taps"):
        fetches["weights"].wait()
        set_taps(0)

    def place_shifts(row):
        at = first[0] + row
        x0[0, at], x0[2, at] = shifts(x0[1, at], 1)

    def conv_row(layer, row):
        spacing = 2**layer
        source = inputs[layer]
        window = jnp.concatenate(
            [
                source[b, first[layer] + row + (a - 1) * spacing]
                for a in range(3)
                for b in range(3)
            ],
            axis=0,
        )
        return jnp.dot(taps[layer], window, preferred_element_type=f32)

    def halo_row(layer, row):
        response[base + row] = conv_row(layer, row)

    def fold(values):
        total = values[:, 0:128]
        for at in range(128, cols, 128):
            total = total + values[:, at : at + 128]
        return total

    def late_window(row, which):
        step = 2 ** (LAYERS - 1)
        return jnp.concatenate(
            [x2[b, first[2] + row + (a - 1) * step] for a in which for b in range(3)], axis=0
        )

    def own_row(layer, row, carry, late=False):
        sums, squares = carry
        if late:
            own = part[row] + jnp.dot(
                near_taps[...], late_window(row, (0,)), preferred_element_type=f32
            )
        else:
            own = conv_row(layer, row)
        if layer < LAYERS - 1:
            response[base + row] = own
        else:
            for at in range(chunks):
                here = slice(at * 128, (at + 1) * 128)
                own_ref[at, pl.ds(true_row(row), channels, stride=rows), :] = own[:, here]
        masked = own * masks[0, 0:1, :]
        return sums + fold(masked), squares + fold(masked * own)

    def tally(layer, carry):
        sums, squares = carry
        tally_out[layer, 0:1, 0:channels] = as_row(jnp.sum(sums, axis=1, keepdims=True))
        tally_out[layer, 1:2, 0:channels] = as_row(jnp.sum(squares, axis=1, keepdims=True))
        pixels = jnp.sum(masks[0, 0:1, :], axis=1, keepdims=True) * rows
        tally_out[layer, :, channels:] = jnp.broadcast_to(pixels, (2, 128 - channels))
        tally_in[layer, peers - 1] = tally_out[layer]

    def send_tally(layer):
        order = sorted(range(1, peers), key=lambda step: abs(step - peers // 2))
        for step in order:
            pltpu.make_async_remote_copy(
                src_ref=tally_out.at[layer],
                dst_ref=tally_in.at[layer, peers - 1 - step],
                send_sem=tally_send.at[0],
                recv_sem=tally_recv.at[layer % 2],
                device_id={"rows": lax.rem(me + step, peers)},
                device_id_type=MESH,
            ).start()

    def all_tallies(layer, sem):
        others = tally_in.at[layer, 0 : peers - 1]
        return pltpu.make_async_copy(others, others, sem)

    def take_tally(layer):
        all_tallies(layer, tally_recv.at[layer % 2]).wait()
        total = jnp.sum(tally_in[layer], axis=0)
        count = total[0:1, channels : channels + 1]
        average = total[0:1, 0:channels] / count
        variance = jnp.maximum(total[1:2, 0:channels] / count - average * average, 0.0)
        factor = gains[layer : layer + 1, :] * lax.rsqrt(variance + EPSILON)
        return column(average), column(factor), column(biases[layer : layer + 1, :])

    def finish_row(layer, row, norm):
        average, factor, bias = norm
        which = 0 if 0 <= row < rows else 1 if row < 0 else 2
        scaled = ((response[base + row] - average) * factor + bias).astype(bf16)
        mask = masks[which, 0:1, :].astype(bf16)
        values = jnp.maximum(scaled, jnp.zeros((), bf16)) * mask
        place(inputs[layer + 1], first[layer + 1] + row, values, 2 ** (layer + 1))

    def finish_and_conv(layer, order, norm, carry, ready, waiting):
        step = 2 ** (layer + 1)
        for row in order:
            finish_row(layer, row, norm)
            ready.add(row)
            for out in list(waiting):
                if {out - step, out, out + step} <= ready:
                    carry = own_row(layer + 1, out, carry)
                    waiting.remove(out)
        return carry

    nothing = (jnp.zeros((channels, 128), f32),) * 2

    with scope("b0_conv0_inner"):
        carry = nothing
        for row in range(1, rows - 1):
            carry = own_row(0, row, carry)
        centre = jnp.sum(carry[0], axis=1, keepdims=True) / (
            jnp.sum(masks[0, 0:1, :], axis=1, keepdims=True) * (rows - 2)
        )
        for piece in range(MID, LATE):
            mid_out[piece - MID] = (response[base + piece - 1] - centre).astype(bf16)
        flag_out[7:8, 0:channels] = as_row(centre)
        send_edges(0, (REACH,))
        send_edges(1, (REACH,))
        send_edges(0, (2,), phase == 1)
        set_taps(1)
        set_taps(2)
        split_taps()
    with scope("b1_far"):
        for n in range(len(far) - 1):
            far_wait(n)
            far_signal(n + 1)
    with scope("b2_fast0"):
        take_edges(1, (0,))
        place_shifts(rows)
        carry = own_row(0, rows - 1, carry)
        send_edges(0, (1,), through)
    with scope("b3_take0"):
        take_edges(0, (0,))
    with scope("b4_slow0"):
        place_shifts(-1)
        carry = own_row(0, 0, carry)
    with scope("b5_far"):
        if far:
            far_wait(len(far) - 1)
    with scope("b6_tally0"):
        tally(0, carry)
        send_tally(0)
        send_edges(0, (3, 4), phase == 1)
        send_edges(0, (2, 3, 4), phase == 2)
        send_edges(0, (2,), through)
    with scope("b7_fast12"):
        fetches["gain"].wait()
        fetches["bias"].wait()
        rest = x0.at[1, REACH + rows + 1 : 2 * REACH + rows]
        if_there(1, lambda: pltpu.make_async_copy(rest, rest, edge_recv.at[2]).wait())
        for piece in range(1, REACH):
            place_shifts(rows + piece)
        for piece in (1, 2):
            halo_row(0, rows - 1 + piece)
    with scope("b8_take1"):
        take_edges(0, (1,))
        flags_done(edge_recv.at[0])
    with scope("b8_slow1"):
        masks[1] = widen(flag_in[0])
        masks[2] = widen(flag_in[1])
        place_shifts(-2)
        halo_row(0, -1)
    with scope("b8_fast"):
        for piece in range(3, REACH):
            halo_row(0, rows - 1 + piece)
        send_edges(0, (3,), through)
    with scope("c0_take_tally0"):
        norm0 = take_tally(0)
        all_tallies(0, tally_send.at[0]).wait()
        near_centre = column(flag_in[0, 7:8, 0:channels])
        send_edges(0, (4,), through)

    def take_mid(piece):
        with scope(f"d{piece}_take"):
            take_edges(0, (piece,))
        response[base - piece] = mid_in[piece - MID].astype(f32) + near_centre

    take_mid(2)
    with scope("c1_layer1"):
        ready, waiting = set(), list(range(rows))
        order = (3, 5, 7, 2, 4, 6, rows, rows + 1, 1, 0, -1, -2)
        carry = finish_and_conv(0, order, norm0, nothing, ready, waiting)
        assert not waiting
    with scope("c2_tally1"):
        tally(1, carry)
        send_tally(1)
    with scope("c3_late"):
        sums = jnp.sum(carry[0], axis=1, keepdims=True)
        pixels = jnp.sum(masks[0, 0:1, :], axis=1, keepdims=True) * rows
        centre = sums / pixels
        for piece in range(LATE, REACH):
            late_out[piece - LATE] = (response[base + piece - 3] - centre).astype(bf16)
            send_edges(0, (piece,), direct)
    with scope("d0_fast"):
        for piece in range(3, REACH):
            finish_row(0, rows - 1 + piece, norm0)
        for piece in range(3, REACH):
            halo_row(1, rows - 3 + piece)

    def slow_piece(piece):
        take_mid(piece)
        with scope(f"d{piece}_work"):
            finish_row(0, -piece, norm0)
            halo_row(1, 2 - piece)

    send_edges(0, (LATE,), through)
    slow_piece(3)
    slow_piece(4)
    send_edges(0, range(LATE + 1, REACH), through)
    with scope("e0_take_tally1"):
        norm1 = take_tally(1)
        all_tallies(1, tally_send.at[0]).wait()
    ready, waiting = set(), list(range(rows))
    with scope("e1_layer2"):
        order = (11, 7, 3, -1, 10, 6, 2, -2, 9, 5, 1, 8, 4, 0)
        carry = finish_and_conv(1, order, norm1, nothing, ready, waiting)
        for row in waiting:
            part[row] = jnp.dot(
                rest_taps[...], late_window(row, (1, 2)), preferred_element_type=f32
            )
        theirs = tally_in[1, jnp.where(odd == 1, 0, peers - 2)]
        centre = column(theirs[0:1, 0:channels] / theirs[0:1, channels : channels + 1])
    for piece in range(LATE, REACH):
        with scope(f"e{piece}_take"):
            take_edges(0, (piece,))
        with scope(f"e{piece}_late"):
            row = 2 - piece
            response[base + row] = late_in[piece - LATE].astype(f32) + centre
            finish_row(1, row, norm1)
            carry = own_row(2, row + 4, carry, late=True)
            waiting.remove(row + 4)
    assert not waiting
    with scope("e7_tally2"):
        tally(2, carry)
    with scope("e7_send"):
        send_tally(2)
    with scope("e8_sent"):
        sent = x0.at[1, 0:REACH]
        for side in range(2):
            if_there(side, lambda: pltpu.make_async_copy(sent, sent, edge_send.at[side]).wait())
        flags_done(edge_send.at[2])
        all_tallies(2, tally_send.at[0]).wait()
    with scope("f0_take_tally2"):
        norm2 = take_tally(2)
    with scope("f1_norm"):
        for n in range(3):
            norm_ref[n] = jnp.broadcast_to(norm2[n], (channels, 128))


def finish(own_ref, norm_ref, mask_ref, out_ref, result, sems):
    channels, rows, cols = out_ref.shape
    part = channels // sems.shape[0]
    masks = [
        jnp.broadcast_to(mask_ref[0:1, at : at + 128], (rows, 128)) for at in range(0, cols, 128)
    ]
    copies = []
    for n in range(sems.shape[0]):
        for channel in range(n * part, (n + 1) * part):
            average, factor, bias = (norm_ref[k, channel : channel + 1, :] for k in range(3))
            for at, mask in enumerate(masks):
                scaled = (own_ref[at, channel * rows : (channel + 1) * rows, :] - average) * factor
                values = jnp.maximum(scaled + bias, 0.0) * mask
                result[channel, :, at * 128 : (at + 1) * 128] = values.astype(result.dtype)
        here = pl.ds(n * part, part)
        copy = pltpu.make_async_copy(result.at[here], out_ref.at[here], sems.at[n])
        copy.start()
        copies.append(copy)
    for copy in copies:
        copy.wait()


def per_device(peers, *arrays):
    channels, rows, cols = arrays[0].shape
    assert rows == TILE and rows > REACH and arrays[1].shape[0] == 1 and channels < 128
    f32, bf16 = jnp.float32, jnp.bfloat16
    vmem = pl.BlockSpec(memory_space=pltpu.VMEM)
    hbm = pl.BlockSpec(memory_space=pltpu.HBM)
    own, norm, mask = pl.pallas_call(
        functools.partial(stack, peers),
        out_shape=(
            jax.ShapeDtypeStruct((cols // 128, channels * rows, 128), f32),
            jax.ShapeDtypeStruct((3, channels, 128), f32),
            jax.ShapeDtypeStruct((8, cols), f32),
        ),
        in_specs=[hbm] * 7,
        out_specs=(vmem,) * 3,
        scratch_shapes=[
            pltpu.VMEM((channels, rows, cols), bf16),
            pltpu.VMEM(arrays[1].shape, jnp.int32),
            pltpu.VMEM(arrays[2].shape, jnp.int32),
            pltpu.VMEM(arrays[3].shape, f32),
            pltpu.VMEM(arrays[5].shape, f32),
            pltpu.VMEM(arrays[6].shape, f32),
            pltpu.VMEM(arrays[4].shape, bf16),
            pltpu.VMEM((cols // 128, channels * rows, 128), f32),
            pltpu.VMEM((channels, cols), f32),
            pltpu.VMEM((3, rows + 2 * REACH, channels, cols), bf16),
            pltpu.VMEM((3, rows + 2 * (REACH - 1), channels, cols), bf16),
            pltpu.VMEM((3, rows + 2 * (REACH - 3), channels, cols), bf16),
            pltpu.VMEM((rows + 2 * (REACH - 1), channels, cols), f32),
            pltpu.VMEM((LATE - MID, channels, cols), bf16),
            pltpu.VMEM((LATE - MID, channels, cols), bf16),
            pltpu.VMEM((REACH - LATE, channels, cols), bf16),
            pltpu.VMEM((REACH - LATE, channels, cols), bf16),
            pltpu.VMEM((REACH - LATE, channels, cols), f32),
            pltpu.VMEM((channels, 3 * channels), bf16),
            pltpu.VMEM((channels, 6 * channels), bf16),
            pltpu.VMEM((LAYERS, channels, 9 * channels), bf16),
            pltpu.VMEM((3, 8, cols), f32),
            pltpu.VMEM((8, 128), f32),
            pltpu.VMEM((2, 8, 128), f32),
            pltpu.VMEM((LAYERS, 2, 128), f32),
            pltpu.VMEM((LAYERS, peers, 2, 128), f32),
            pltpu.SemaphoreType.DMA((3,)),
            pltpu.SemaphoreType.DMA((3 + LATE,)),
            pltpu.SemaphoreType.DMA((1,)),
            pltpu.SemaphoreType.DMA((2,)),
            pltpu.SemaphoreType.DMA((5,)),
            pltpu.SemaphoreType.REGULAR((max(len(rounds(peers)), 1),)),
        ],
        compiler_params=pltpu.CompilerParams(
            collective_id=0, has_side_effects=True, vmem_limit_bytes=44 * 2**20
        ),
    )(*(pltpu.with_memory_space_constraint(array, pltpu.HBM) for array in arrays))
    return pl.pallas_call(
        finish,
        out_shape=jax.ShapeDtypeStruct((channels, rows, cols), bf16),
        in_specs=[vmem] * 3,
        out_specs=pl.BlockSpec(memory_space=pl.ANY),
        scratch_shapes=[
            pltpu.VMEM((channels, rows, cols), bf16),
            pltpu.SemaphoreType.DMA((4 if channels % 4 == 0 else 1,)),
        ],
        compiler_params=pltpu.CompilerParams(vmem_limit_bytes=8 * 2**20),
    )(own, norm, mask)


def solution(mesh):
    banded = P(None, ("groups", "rows"), None)
    tiled = P(("groups", "rows"), None)
    return jax.shard_map(
        functools.partial(per_device, mesh.shape["rows"]),
        mesh=mesh,
        in_specs=(banded, tiled, tiled, P(), P(), P(), P()),
        out_specs=banded,
        check_vma=False,
    )
```
